32 devices in a mesh: rep: 2 (over y), pipe: 2 (over core), tp: 8 (over z, x).
Axes of the slice: x: 2, y: 2, z: 4, core: 2. Of those that a mesh axis runs over, the one named last changes fastest.
Arguments:
- hidden_entering: bfloat16 [2, 120, 8192], P('rep', None, 'tp'), parts along dimension 0, may hold values from -60 to 60
- segment_adapter: int32 [2, 3], P('rep'), parts along dimension 0, may hold values from 0 to 127, as said below
- segment_requests: int32 [2, 3], P('rep'), parts along dimension 0, may hold values from 10 to 40, as said below
- section_norm_gain: float32 [2, 8192], P('pipe'), may hold values from 0.25 to 1.75
- up_matrix: bfloat16 [2, 14336, 8192], P('pipe', 'tp'), may hold values from -0.0625 to 0.0625
- down_matrix: bfloat16 [2, 8192, 14336], P('pipe', 'tp'), may hold values from -0.046875 to 0.046875
- adapter_reduce: bfloat16 [2, 128, 131072], P('pipe', None, 'tp'), may hold values from -0.0625 to 0.0625
- adapter_expand: bfloat16 [2, 128, 229376], P('pipe', None, 'tp'), may hold values from -1.5 to 1.5
Outputs:
- section_out: bfloat16 [2, 2, 120, 8192], P('pipe', 'rep', None, 'tp'), parts along dimension 1
The draws below stay inside these ranges and needn't reach their ends.
There are 2 independent parts, one for each index of `rep`. The reference program is written for one: setup_inputs(seed, part) draws one part's arguments, and reference() takes and returns one part's arrays. A program takes and returns all parts, laid end to end along the dimension named above; an argument that names none is the same for every part. Nothing has to cross between parts.
Inputs may be any that keep to these rules, and one draw needn't show every extreme that they name: `segment_adapter`: within each micro-batch the adapter ids of its segments do not decrease. The first segment_requests[m, j] rows of segment j of micro-batch m hold requests; the other rows are padding.
All inputs are finite; a program needn't handle non-finite values.
Results may differ from the reference program's by a relative error of at most 0.0045.
Values may be sent and summed in bfloat16 or wider, within the bound.
A program may use at most 128 MiB of HBM per device.

```python
import math
import jax
import jax.numpy as jnp
from jax import lax

MODEL_DIMENSION = 8192
FEEDFORWARD_UNITS = 14336
ADAPTER_RANK = 16
ADAPTER_COUNT = 128
SEG = 40
SPM = 3
MB = 1
N_PIPE = 2


def draw_hidden_entering(key, part):
    row_count = SPM * SEG
    keys = jax.random.split(jax.random.fold_in(key, 101), 3)
    row_scale = jnp.exp(jax.random.uniform(keys[0], (MB, row_count, 1), jnp.float32, math.log(0.4), math.log(4.0)))
    rising = jnp.exp(math.log(3.0) * jnp.arange(MODEL_DIMENSION, dtype=jnp.float32) / MODEL_DIMENSION)
    col_scale = jnp.exp(jax.random.uniform(keys[1], (MODEL_DIMENSION,), jnp.float32, math.log(0.4), math.log(4.0))) * rising / 1.7
    values = jax.random.normal(keys[2], (MB, row_count, MODEL_DIMENSION), jnp.float32)
    return jnp.clip(values * row_scale * col_scale, -60.0, 60.0).astype(jnp.bfloat16)


def draw_segment_adapter(key, part):
    raw = jax.random.randint(jax.random.fold_in(key, 7), (MB, SPM), 0, ADAPTER_COUNT)
    return jnp.sort(raw, axis=-1).astype(jnp.int32)


def draw_segment_requests(key, part):
    keys = jax.random.split(jax.random.fold_in(key, 13), 2)
    counts = jax.random.randint(keys[0], (MB * SPM,), SEG // 4, SEG + 1)
    chosen = jax.random.randint(keys[1], (), 0, MB * SPM)
    counts = jnp.where(jnp.arange(MB * SPM) == chosen, SEG, counts)
    return counts.reshape(MB, SPM).astype(jnp.int32)


def level_of(key, dims, cuts, least, largest):
    def one(position, shards_of):
        steps = jax.random.uniform(jax.random.fold_in(jax.random.fold_in(key, 6), position), (shards_of,), jnp.float32, least / len(cuts), largest / len(cuts))
        return jnp.repeat(jnp.exp(steps), dims[position] // shards_of).reshape((-1,) + (1,) * (len(dims) - position - 1))

    factor_of = one(*cuts[0])
    for cut in cuts[1:]:
        factor_of = factor_of * one(*cut)
    return factor_of


def bell_draw(key, extent, spread, most, shards=(), kind=jnp.bfloat16):
    loudness = level_of(key, extent, shards, -0.22, 0.18) if shards else 1.0
    entries = jax.random.normal(key, extent, jnp.float32) * spread * loudness
    return jnp.minimum(jnp.maximum(entries, -most), most).astype(kind)


def setup_inputs(seed: int = 0, part: int = 0) -> dict:
    seeds = jax.random.split(jax.random.key(seed), 9)
    part_keys = jax.random.split(jax.random.fold_in(seeds[8], part), 9)
    hidden_entering = draw_hidden_entering(jax.random.fold_in(jax.random.fold_in(seeds[8], part), 71), part)
    segment_adapter = draw_segment_adapter(jax.random.fold_in(jax.random.fold_in(seeds[8], part), 71), part)
    segment_requests = draw_segment_requests(jax.random.fold_in(jax.random.fold_in(seeds[8], part), 71), part)
    section_norm_gain = jnp.clip(1.0 + 0.15 * jax.random.normal(seeds[3], (N_PIPE, MODEL_DIMENSION), jnp.float32), 0.25, 1.75)
    up_matrix = bell_draw(seeds[4], (N_PIPE, FEEDFORWARD_UNITS, MODEL_DIMENSION), MODEL_DIMENSION ** -0.5, 0.0625, ((0, 2), (1, 8)))
    down_matrix = bell_draw(seeds[5], (N_PIPE, MODEL_DIMENSION, FEEDFORWARD_UNITS), FEEDFORWARD_UNITS ** -0.5, 0.046875, ((0, 2), (1, 8)))
    adapter_reduce = bell_draw(seeds[6], (N_PIPE, ADAPTER_COUNT, MODEL_DIMENSION * ADAPTER_RANK), MODEL_DIMENSION ** -0.5, 0.0625, ((0, 2), (2, 8)))
    adapter_expand = bell_draw(seeds[7], (N_PIPE, ADAPTER_COUNT, FEEDFORWARD_UNITS * ADAPTER_RANK), ADAPTER_RANK ** -0.5, 1.5, ((0, 2), (2, 8)))
    return dict(hidden_entering=hidden_entering, segment_adapter=segment_adapter, segment_requests=segment_requests, section_norm_gain=section_norm_gain, up_matrix=up_matrix, down_matrix=down_matrix, adapter_reduce=adapter_reduce, adapter_expand=adapter_expand)


EPSILON = 1e-05

def times_rows(left, weight):
    return lax.dot_general(left, weight, (((1,), (1,)), ((), ())), preferred_element_type=jnp.float32)

def apply_section(hidden_flow, section_ordinal, segment_adapter, segment_requests, section_norm_gain, up_matrix, down_matrix, adapter_reduce, adapter_expand):
    batch_list = hidden_flow.shape[0]
    row_count = hidden_flow.shape[1]
    feature_width = hidden_flow.shape[2]
    hidden_extent = up_matrix.shape[1]
    batch_results = segment_adapter.shape[1]
    seg_rows = row_count // batch_results
    adapter_rank_count = adapter_reduce.shape[2] // feature_width
    widened = hidden_flow.astype(jnp.float32)
    scaled = (widened * section_norm_gain[section_ordinal]).astype(jnp.bfloat16)
    inverse = lax.rsqrt(lax.optimization_barrier(jnp.mean(widened * widened, axis=-1, keepdims=True)) + EPSILON)
    flat_scaled = scaled.reshape(batch_list * row_count, feature_width)
    base_up = times_rows(flat_scaled, up_matrix[section_ordinal]).reshape(batch_list, row_count, hidden_extent)
    input_panel = adapter_reduce[section_ordinal][segment_adapter].reshape(batch_list, batch_results, feature_width, adapter_rank_count).astype(jnp.float32)
    output_panel = adapter_expand[section_ordinal][segment_adapter].reshape(batch_list, batch_results, hidden_extent, adapter_rank_count).astype(jnp.float32)
    segment_scaled = scaled.reshape(batch_list, batch_results, seg_rows, feature_width).astype(jnp.float32)
    shrunk = jnp.einsum('msdr,mspd->msrp', input_panel, segment_scaled)
    low_rank = (inverse.reshape(batch_list, batch_results, 1, seg_rows) * shrunk).astype(jnp.bfloat16)
    adapted = jnp.einsum('msrp,msdr->mspd', low_rank.astype(jnp.float32), output_panel).reshape(batch_list, row_count, hidden_extent)
    up_sum = inverse * base_up + adapted
    hidden_act = jax.nn.silu(up_sum).astype(jnp.bfloat16)
    down_sum = times_rows(hidden_act.reshape(batch_list * row_count, hidden_extent), down_matrix[section_ordinal]).reshape(batch_list, row_count, feature_width)
    updated = (widened + down_sum).astype(jnp.bfloat16)
    positions = lax.broadcasted_iota(jnp.int32, (batch_list, batch_results, seg_rows), 2)
    row_kept = (positions < segment_requests[:, :, None]).reshape(batch_list, row_count, 1)
    return jnp.where(row_kept, updated, jnp.zeros_like(updated))

def reference(hidden_entering, segment_adapter, segment_requests, section_norm_gain, up_matrix, down_matrix, adapter_reduce, adapter_expand):
    hidden_flow = hidden_entering
    outputs = []
    for section_ordinal in range(N_PIPE):
        hidden_flow = apply_section(hidden_flow, section_ordinal, segment_adapter, segment_requests, section_norm_gain, up_matrix, down_matrix, adapter_reduce, adapter_expand)
        outputs.append(hidden_flow)
    return jnp.stack(outputs)
```

```python
import functools

import jax
import jax.numpy as jnp
from jax import lax
from jax.experimental import pallas as pl
from jax.experimental.pallas import tpu as pltpu
from jax.sharding import PartitionSpec as P

EPSILON = 1e-05


def shifted(x, axis, by):
    size = lax.axis_size(axis)
    pairs = [(i, i + by) for i in range(size) if 0 <= i + by < size]
    return lax.ppermute(x, axis, pairs)


def times_rows(left, weight):
    return lax.dot_general(
        left, weight, (((1,), (1,)), ((), ())), preferred_element_type=jnp.float32
    )


def block_step(
    current, unit_ids, unit_live, gain_full, up_weight, down_weight, shrink_weight, expand_weight
):
    row_count = current.shape[0]
    col_count = current.shape[1]
    hid_count = up_weight.shape[0]
    segments = unit_ids.shape[0]
    seg_rows = row_count // segments
    feature_width = gain_full.shape[0]
    adapter_rank_count = shrink_weight.shape[1] // col_count
    column = lax.axis_index("tp") * col_count
    gain_mine = lax.dynamic_slice_in_dim(gain_full, column, col_count, 0)
    widened_local = current.astype(jnp.float32)
    local_scaled = (widened_local * gain_mine).astype(jnp.bfloat16)
    input_panel = shrink_weight[unit_ids].reshape(segments, col_count, adapter_rank_count)
    output_panel = expand_weight[unit_ids].reshape(segments, hid_count, adapter_rank_count)
    partial_value = jnp.einsum(
        "sdr,spd->rsp",
        input_panel,
        local_scaled.reshape(segments, seg_rows, col_count),
        preferred_element_type=jnp.float32,
    ).reshape(adapter_rank_count, row_count)
    local_squares = jnp.sum(widened_local * widened_local, axis=1)
    reduced, squares = lax.psum((partial_value, local_squares), "tp")
    widened = lax.all_gather(current, "tp", axis=1, tiled=True).astype(jnp.float32)
    scaled = (widened * gain_full).astype(jnp.bfloat16)
    up_total = times_rows(scaled, up_weight)
    inverse = lax.rsqrt(squares / feature_width + EPSILON)
    low_rank = (
        (reduced * inverse[None, :])
        .astype(jnp.bfloat16)
        .reshape(adapter_rank_count, segments, seg_rows)
    )
    adapted = jnp.einsum(
        "rsp,sdr->spd", low_rank, output_panel, preferred_element_type=jnp.float32
    ).reshape(row_count, hid_count)
    up_sum = inverse[:, None] * up_total + adapted
    hidden_act = jax.nn.silu(up_sum).astype(jnp.bfloat16)
    down_sum = times_rows(lax.all_gather(hidden_act, "tp", axis=1, tiled=True), down_weight)
    updated = (widened_local + down_sum).astype(jnp.bfloat16)
    positions = lax.broadcasted_iota(jnp.int32, (segments, seg_rows), 1)
    row_kept = (positions < unit_live[:, None]).reshape(row_count, 1)
    return jnp.where(row_kept, updated, jnp.zeros_like(updated))


MESH = pl.DeviceIdType.MESH
PIECE = 256
COLUMNS = 2
LANES = 128
VMEM_BYTES = 67_043_328
NT = (((1,), (1,)), ((), ()))


class Spread:
    def __init__(self, buf, send, recv, pieces, z, x, depth, starts_own):
        self.buf, self.send, self.recv, self.pieces = buf, send, recv, pieces
        self.z, self.x, self.depth, self.starts_own = z, x, depth, starts_own
        self.shards = depth * COLUMNS
        self.me = z * COLUMNS + x

    def copy(self, t, c, way, target):
        return pltpu.make_async_remote_copy(
            src_ref=self.buf.at[t, c], dst_ref=self.buf.at[t, c],
            send_sem=self.send.at[way, t, c], recv_sem=self.recv.at[t, c],
            device_id={"tp": target}, device_id_type=MESH)

    def each(self, source_z, column, c, do):
        z, x, me = self.z, self.x, self.me
        t = source_z * COLUMNS + column
        own, special = column == x, c == self.pieces - 1
        along = jnp.logical_or(own, special)
        across = jnp.logical_and(own, jnp.logical_or(c != self.pieces - 1, source_z == z))

        @pl.when(jnp.logical_and(along, jnp.logical_and(source_z <= z, z < self.depth - 1)))
        def _():
            do(self.copy(t, c, 0, (me + COLUMNS) % self.shards))

        @pl.when(jnp.logical_and(along, jnp.logical_and(source_z >= z, z > 0)))
        def _():
            do(self.copy(t, c, 1, (me + self.shards - COLUMNS) % self.shards))

        @pl.when(across)
        def _():
            do(self.copy(t, c, 2, z * COLUMNS + (1 - x)))

    def forward(self, source_z, column, c):
        self.each(source_z, column, c, lambda d: d.start())

    def arrive(self, t, c):
        self.copy(t, c, 2, self.z * COLUMNS + (1 - self.x)).wait_recv()

    def relay(self, step, column, c):
        for source_z in (self.z - step, self.z + step) if step else (self.z,):
            @pl.when(jnp.logical_and(source_z >= 0, source_z < self.depth))
            def _():
                self.arrive(source_z * COLUMNS + column, c)
                self.forward(source_z, column, c)

    def drain(self):
        @pl.loop(0, self.depth)
        def _(source_z):
            @pl.when(jnp.logical_or(source_z != self.z, self.starts_own))
            def _():
                @pl.loop(0, self.pieces)
                def _(c):
                    self.each(source_z, self.x, c, lambda d: d.wait_send())

            self.each(source_z, 1 - self.x, self.pieces - 1, lambda d: d.wait_send())


def section_kernel(
    ids_ref, live_ref, gain_ref, x_hbm, reduce_hbm, expand_hbm, up_hbm, down_hbm, out_ref,
    up_v, down_v, xs, act, acc, sq, shrink, expand, partial,
    up_sem, down_sem, tab_sem, own_sem, part_send, part_recv, x_send, x_recv, a_send, a_recv, h_send,
):
    shards, x_pieces, rows, _ = xs.shape
    a_pieces = act.shape[1]
    cols = x_pieces * PIECE
    hidden = up_v.shape[0]
    width = shards * cols
    adapters, shrink_len = reduce_hbm.shape
    expand_len = expand_hbm.shape[1]
    segments = ids_ref.shape[0]
    rank = shrink_len // cols
    table_width = shards * hidden // (PIECE * rank) * (PIECE * rank)
    seg_rows = rows // segments
    depth = shards // COLUMNS
    me = lax.axis_index("tp")
    stage = lax.axis_index("pipe")
    stages = lax.axis_size("pipe")
    z, x = me // COLUMNS, me % COLUMNS
    partner = z * COLUMNS + (1 - x)
    upper = (me + COLUMNS) % shards
    lower = (me + shards - COLUMNS) % shards
    f32, bf16 = jnp.float32, jnp.bfloat16

    few = jnp.minimum(z, depth - 1 - z)
    layer = [z]
    for i in range(1, depth):
        both = i <= 2 * few
        far = jnp.where(both, (i + 1) // 2, i - few)
        down_side = jnp.where(both, i % 2 == 1, z > depth - 1 - z)
        layer.append(jnp.where(down_side, z - far, z + far))

    def shard(i, other):
        return layer[i] * COLUMNS + ((1 - x) if other else x)

    visits = [shard(i, other) for i in range(depth) for other in (False, True)]

    def up_copy(t):
        span = pl.ds(pl.multiple_of(t * cols, LANES), cols)
        return pltpu.make_async_copy(up_hbm.at[:, span], up_v.at[:, span], up_sem.at[t])

    def down_copy(t):
        span = pl.ds(pl.multiple_of(t * hidden, LANES), hidden)
        return pltpu.make_async_copy(down_hbm.at[:, span], down_v.at[:, span], down_sem.at[t])

    def own_copy(c):
        return pltpu.make_async_copy(x_hbm.at[:, c * PIECE:(c + 1) * PIECE], xs.at[me, c], own_sem.at[c])

    tables = []
    for table, length in ((reduce_hbm, shrink_len), (expand_hbm, expand_len)):
        blocks = []
        for at in range(0, length, table_width):
            size = min(table_width, length - at)
            k = sum(len(t) for t in tables) + len(blocks)
            copy = pltpu.make_async_copy(
                table.at[:, at:at + size],
                down_v.at[k * adapters:(k + 1) * adapters, 0:size], tab_sem.at[k])
            blocks.append((k, size, copy))
        tables.append(blocks)

    @pl.when(stage == 0)
    def _():
        for c in range(x_pieces):
            own_copy(c).start()

    up_copy(me).start()
    for blocks in tables:
        for _k, _size, copy in blocks:
            copy.start()
    for t in visits[1:]:
        up_copy(t).start()

    barrier = pltpu.get_barrier_semaphore()

    @pl.loop(1, shards)
    def _(i):
        pl.semaphore_signal(barrier, inc=1, device_id={"tp": (me + i) % shards}, device_id_type=MESH)

    def greet(target):
        pl.semaphore_signal(
            barrier, inc=1, device_id={"pipe": stage - 1, "tp": target}, device_id_type=MESH)

    @pl.when(stage > 0)
    def _():
        greet(me)
        greet(partner)

        @pl.when(z < depth - 1)
        def _():
            greet(upper)

        @pl.when(z > 0)
        def _():
            greet(lower)

    fed = 2 + jnp.where(z < depth - 1, 1, 0) + jnp.where(z > 0, 1, 0)
    pl.semaphore_wait(barrier, shards - 1 + jnp.where(stage < stages - 1, fed, 0))

    x_side = Spread(xs, x_send, x_recv, x_pieces, z, x, depth, stage == 0)
    a_side = Spread(act, a_send, a_recv, a_pieces, z, x, depth, stage >= 0)

    def hand_over(c, way, target):
        return pltpu.make_async_remote_copy(
            src_ref=out_ref.at[c], dst_ref=xs.at[me, c],
            send_sem=h_send.at[way, c], recv_sem=x_recv.at[me, c],
            device_id={"pipe": (stage + 1) % stages, "tp": target}, device_id_type=MESH)

    def hand_each(c, do):
        @pl.when(stage < stages - 1)
        def _():
            @pl.when(z < depth - 1)
            def _():
                do(hand_over(c, 0, upper))

            @pl.when(z > 0)
            def _():
                do(hand_over(c, 1, lower))

            do(hand_over(c, 2, partner))
            do(hand_over(c, 3, me))

    @pl.when(stage == 0)
    def _():
        for c in range(x_pieces):
            own_copy(c).wait()
            x_side.forward(z, x, c)

    row_seg = lax.broadcasted_iota(jnp.int32, (rows, LANES), 0) // seg_rows
    lane_group = lax.broadcasted_iota(jnp.int32, (rows, LANES), 1) // rank
    in_segment = row_seg == lane_group

    picks = jnp.zeros((8 * segments, adapters), f32)
    pick_row = lax.broadcasted_iota(jnp.int32, picks.shape, 0)
    pick_col = lax.broadcasted_iota(jnp.int32, picks.shape, 1)
    for s in range(segments):
        hit = jnp.logical_and(pick_row // 8 == s, pick_col == ids_ref[s])
        picks = jnp.where(hit, 1.0, picks)
    picks = picks.astype(bf16)
    flat = PIECE * rank
    lane_tiles = flat // LANES
    spot_row = lax.broadcasted_iota(jnp.int32, (PIECE, LANES), 0) % 8
    spot_lane = lax.broadcasted_iota(jnp.int32, (PIECE, LANES), 1) // rank
    spot = spot_row == spot_lane
    fold_row = lax.broadcasted_iota(jnp.int32, (segments * LANES, LANES), 0)
    fold_col = lax.broadcasted_iota(jnp.int32, (segments * LANES, LANES), 1)
    fold = jnp.where(fold_col == fold_row // LANES * rank + fold_row % rank, 1.0, 0.0).astype(bf16)

    for blocks in tables:
        for _k, _size, copy in blocks:
            copy.wait()
    for blocks, dest in zip(tables, (shrink, expand)):
        done = 0
        for k, size, copy in blocks:
            first = done

            @pl.loop(0, size // flat)
            def _(j):
                span = pl.ds(pl.multiple_of(j * flat, LANES), flat)
                table = down_v[k * adapters:(k + 1) * adapters, span]
                got = jnp.dot(picks, table, preferred_element_type=f32)
                parts = []
                for s in range(segments):
                    tall = jnp.concatenate(
                        [got[8 * s:8 * s + 8, LANES * i:LANES * (i + 1)] for i in range(lane_tiles)], axis=0)
                    parts.append(jnp.where(spot, tall, 0.0).astype(bf16))
                panel = jnp.dot(jnp.concatenate(parts, axis=1), fold, preferred_element_type=f32)
                at = pl.multiple_of((first + j) * PIECE, PIECE)
                dest[pl.ds(at, PIECE), :] = panel.astype(bf16)

            done += size // flat

    for t in visits:
        down_copy(t).start()

    def raw(t, c):
        return xs[t, c].astype(f32)

    def scaled(t, c, wide):
        at = pl.multiple_of(t * cols + c * PIECE, LANES)
        return (wide * gain_ref[:, pl.ds(at, PIECE)]).astype(bf16)

    def squares(wide):
        square = wide * wide
        return square[:, :LANES] + square[:, LANES:]

    def up_tile(n, t, c):
        at = pl.multiple_of(t * cols + c * PIECE, LANES)
        return up_v[n * PIECE:(n + 1) * PIECE, pl.ds(at, PIECE)]

    def up_add(items, init):
        lefts = []
        total = jnp.zeros((rows, LANES), f32) if init else sq[...]
        for t, c in items:
            wide = raw(t, c)
            total += squares(wide)
            lefts.append(scaled(t, c, wide))
        sq[...] = total
        for n in range(a_pieces):
            block = slice(n * PIECE, (n + 1) * PIECE)
            part = jnp.zeros((rows, PIECE), f32)
            for (t, c), left in zip(items, lefts):
                part += lax.dot_general(left, up_tile(n, t, c), NT, preferred_element_type=f32)
            acc[:, block] = part if init else acc[:, block] + part

    @pl.when(stage > 0)
    def _():
        for c in range(x_pieces):
            x_side.arrive(me, c)

    up_copy(me).wait()
    up_add([(me, c) for c in range(x_pieces)], True)

    def part_copy(owner, target):
        return pltpu.make_async_remote_copy(
            src_ref=partial.at[owner], dst_ref=partial.at[owner], send_sem=part_send.at[target],
            recv_sem=part_recv.at[owner], device_id={"tp": target}, device_id_type=MESH)

    low = jnp.zeros((rows, LANES), f32)
    for c in range(x_pieces):
        low += jnp.dot(scaled(me, c, raw(me, c)), shrink[c * PIECE:(c + 1) * PIECE, :],
                       preferred_element_type=f32)
    low = jnp.where(in_segment, low, 0.0)
    if rows < LANES:
        low = jnp.concatenate([low, jnp.zeros((LANES - rows, LANES), f32)], axis=0)
    turned = jnp.transpose(low)
    picked = turned[0:rank]
    for s in range(1, segments):
        picked = picked + turned[s * rank:(s + 1) * rank]
    partial[me] = picked

    @pl.loop(1, shards)
    def _(i):
        part_copy(me, (me + i) % shards).start()

    def spread_in(side, step, weights, pieces_of, add):
        for t in weights:
            t.wait()

        @pl.loop(0, side.pieces)
        def _(c):
            side.relay(step, x, c)

            @pl.when(c < side.pieces - 1)
            def _():
                side.arrive(shard(step - 1, True), c)

            @pl.when(c == side.pieces - 1)
            def _():
                side.relay(step - 1, 1 - x, c)

            add([(t, c) for t in pieces_of])

    for i in range(1, depth):
        fresh = [shard(i - 1, True), shard(i, False)]
        spread_in(x_side, i, [up_copy(t) for t in fresh], fresh, lambda items: up_add(items, False))

    last = shard(depth - 1, True)
    up_copy(last).wait()

    @pl.loop(0, x_pieces - 2)
    def _(c):
        x_side.arrive(last, c)
        up_add([(last, c)], False)

    @pl.loop(1, shards)
    def _(i):
        owner = (me + i) % shards
        part_copy(owner, owner).wait_recv()

    summed = partial[0]
    for t in range(1, shards):
        summed = summed + partial[t]
    stacked = jnp.concatenate([summed] * segments + [jnp.zeros((LANES - segments * rank, LANES), f32)], axis=0)
    low = jnp.where(in_segment, jnp.transpose(stacked)[:rows], 0.0)

    x_side.arrive(last, x_pieces - 2)
    x_side.relay(depth - 1, 1 - x, x_pieces - 1)
    finals = [(last, x_pieces - 2), (last, x_pieces - 1)]
    square = sq[...]
    lefts = []
    for t, c in finals:
        wide = raw(t, c)
        square += squares(wide)
        lefts.append(scaled(t, c, wide))
    inverse = lax.rsqrt(jnp.sum(square, axis=1, keepdims=True) / width + EPSILON)
    low_rank = (low * inverse).astype(bf16)

    for n in range(a_pieces):
        block = slice(n * PIECE, (n + 1) * PIECE)
        base = jnp.zeros((rows, PIECE), f32)
        for (t, c), left in zip(finals, lefts):
            base += lax.dot_general(left, up_tile(n, t, c), NT, preferred_element_type=f32)
        adapted = lax.dot_general(low_rank, expand[block, :], NT, preferred_element_type=f32)
        value = inverse * (acc[:, block] + base) + adapted
        act[me, n] = (value / (1.0 + jnp.exp(-value))).astype(bf16)
        a_side.forward(z, x, n)

    def down_tile(n, t, c):
        at = pl.multiple_of(t * hidden + c * PIECE, LANES)
        return down_v[n * PIECE:(n + 1) * PIECE, pl.ds(at, PIECE)]

    def down_add(items):
        for n in range(x_pieces):
            block = slice(n * PIECE, (n + 1) * PIECE)
            part = jnp.zeros((rows, PIECE), f32)
            for t, c in items:
                part += lax.dot_general(act[t, c], down_tile(n, t, c), NT, preferred_element_type=f32)
            acc[:, block] = acc[:, block] + part

    for n in range(x_pieces):
        acc[:, n * PIECE:(n + 1) * PIECE] = xs[me, n].astype(f32)

    down_copy(me).wait()
    for i in range(1, depth):
        fresh = [shard(i - 1, True), shard(i, False)]
        spread_in(a_side, i, [down_copy(t) for t in fresh],
                  ([me] if i == 1 else []) + fresh, down_add)

    down_copy(last).wait()

    @pl.loop(0, a_pieces - 2)
    def _(c):
        a_side.arrive(last, c)
        down_add([(last, c)])

    row = lax.broadcasted_iota(jnp.int32, (rows, 1), 0)
    kept = row < 0
    for s in range(segments):
        start = s * seg_rows
        kept = jnp.logical_or(kept, jnp.logical_and(row >= start, row < start + jnp.minimum(live_ref[s], seg_rows)))

    a_side.arrive(last, a_pieces - 2)
    a_side.relay(depth - 1, 1 - x, a_pieces - 1)
    for n in range(x_pieces):
        block = slice(n * PIECE, (n + 1) * PIECE)
        part = jnp.zeros((rows, PIECE), f32)
        for c in (a_pieces - 2, a_pieces - 1):
            part += lax.dot_general(act[last, c], down_tile(n, last, c), NT, preferred_element_type=f32)
        out_ref[n] = jnp.where(kept, acc[:, block] + part, 0.0).astype(bf16)
        hand_each(n, lambda d: d.start())

    @pl.loop(0, x_pieces)
    def _(c):
        hand_each(c, lambda d: d.wait_send())

    @pl.loop(1, shards)
    def _(i):
        part_copy(me, (me + i) % shards).wait_send()

    x_side.drain()
    a_side.drain()


def fused_sections(current, ids, live, gain, up_weight, down_weight, shrink_weight, expand_weight):
    rows, cols = current.shape
    hidden = up_weight.shape[0]
    shards = lax.axis_size("tp")
    rank = shrink_weight.shape[1] // cols
    x_pieces, a_pieces = cols // PIECE, hidden // PIECE
    vmem = pl.BlockSpec(memory_space=pltpu.VMEM)
    smem = pl.BlockSpec(memory_space=pltpu.SMEM)
    hbm = pl.BlockSpec(memory_space=pl.ANY)
    dma = pltpu.SemaphoreType.DMA
    flat = PIECE * rank
    blocks = table_blocks(shards * hidden // flat * flat, shrink_weight, expand_weight)
    pieces = pl.pallas_call(
        section_kernel,
        out_shape=jax.ShapeDtypeStruct((x_pieces, rows, PIECE), jnp.bfloat16),
        in_specs=[smem, smem, vmem] + [hbm] * 5,
        out_specs=vmem,
        scratch_shapes=[
            pltpu.VMEM(up_weight.shape, jnp.bfloat16),
            pltpu.VMEM(down_weight.shape, jnp.bfloat16),
            pltpu.VMEM((shards, x_pieces, rows, PIECE), jnp.bfloat16),
            pltpu.VMEM((shards, a_pieces, rows, PIECE), jnp.bfloat16),
            pltpu.VMEM((rows, hidden), jnp.float32),
            pltpu.VMEM((rows, LANES), jnp.float32),
            pltpu.VMEM((cols, LANES), jnp.bfloat16),
            pltpu.VMEM((hidden, LANES), jnp.bfloat16),
            pltpu.VMEM((shards, rank, LANES), jnp.float32),
            dma((shards,)), dma((shards,)), dma((blocks,)), dma((x_pieces,)),
            dma((shards,)), dma((shards,)),
            dma((3, shards, x_pieces)), dma((shards, x_pieces)),
            dma((3, shards, a_pieces)), dma((shards, a_pieces)),
            dma((4, x_pieces)),
        ],
        compiler_params=pltpu.CompilerParams(
            collective_id=0, has_side_effects=True, vmem_limit_bytes=VMEM_BYTES
        ),
    )(ids, live, gain[None, :], current, shrink_weight, expand_weight, up_weight, down_weight)
    return pieces.transpose(1, 0, 2).reshape(rows, cols)


def table_blocks(width, *tables):
    return sum(-(-table.shape[1] // width) for table in tables)


def kernel_fits(row_count, col_count, hidden, segments, shrink_weight, expand_weight):
    shards = lax.axis_size("tp")
    adapters, flat_cols = shrink_weight.shape
    rank = flat_cols // col_count
    flat = PIECE * rank
    width = shards * hidden // flat * flat
    if col_count % PIECE or hidden % PIECE or hidden < 4 * PIECE or col_count < 4 * PIECE:
        return False
    if row_count > LANES or rank * 8 != LANES or segments * rank > LANES or adapters % LANES:
        return False
    if shards % COLUMNS or shards < 2 * COLUMNS or col_count > hidden:
        return False
    if not width or table_blocks(width, shrink_weight, expand_weight) * adapters > col_count:
        return False
    return 2 * hidden * col_count * 2 * shards < VMEM_BYTES - 7 * 2**20


def run_window(
    units, unit_ids, unit_live, gain_full, up_weight, down_weight, shrink_weight, expand_weight
):
    section_index = lax.axis_index("pipe")
    sections = lax.axis_size("pipe")
    unit_count = units.shape[0]
    tick_total = unit_count + sections - 1

    def process(tick_index, received, collected):
        position = jnp.clip(tick_index - section_index, 0, unit_count - 1)
        arriving = lax.dynamic_index_in_dim(
            units, jnp.minimum(tick_index, unit_count - 1), 0, keepdims=False
        )
        current = jnp.where(section_index == 0, arriving, received)
        ids_here = lax.dynamic_index_in_dim(unit_ids, position, 0, keepdims=False)
        live_here = lax.dynamic_index_in_dim(unit_live, position, 0, keepdims=False)
        produced = block_step(
            current,
            ids_here,
            live_here,
            gain_full,
            up_weight,
            down_weight,
            shrink_weight,
            expand_weight,
        )
        lag = tick_index - section_index
        in_window = jnp.logical_and(lag >= 0, lag < unit_count)
        placed = lax.dynamic_update_index_in_dim(collected, produced, position, 0)
        return (produced, jnp.where(in_window, placed, collected))

    def one_tick(tick_index, state):
        produced, collected = process(tick_index, state[0], state[1])
        return (shifted(produced, "pipe", 1), collected)

    start_state = (jnp.zeros_like(units[0]), jnp.zeros_like(units))
    received, collected = lax.fori_loop(0, tick_total - 1, one_tick, start_state)
    produced, collected = process(tick_total - 1, received, collected)
    return collected


def per_device(
    hidden_entering,
    segment_adapter,
    segment_requests,
    section_norm_gain,
    up_matrix,
    down_matrix,
    adapter_reduce,
    adapter_expand,
):
    batch_list = hidden_entering.shape[0]
    row_count = hidden_entering.shape[1]
    col_count = hidden_entering.shape[2]
    hidden = up_matrix.shape[1]
    segments = segment_adapter.shape[1]
    if batch_list == 1 and kernel_fits(
        row_count, col_count, hidden, segments, adapter_reduce[0], adapter_expand[0]
    ):
        produced = fused_sections(
            hidden_entering[0],
            segment_adapter[0],
            segment_requests[0],
            section_norm_gain[0],
            up_matrix[0],
            down_matrix[0],
            adapter_reduce[0],
            adapter_expand[0],
        )
        return produced.reshape(1, batch_list, row_count, col_count)
    collected = run_window(
        hidden_entering,
        segment_adapter,
        segment_requests,
        section_norm_gain[0],
        up_matrix[0],
        down_matrix[0],
        adapter_reduce[0],
        adapter_expand[0],
    )
    return collected.reshape(1, batch_list, row_count, col_count)


def solution(mesh):
    return jax.shard_map(
        per_device,
        mesh=mesh,
        in_specs=(
            P("rep", None, "tp"),
            P("rep", None),
            P("rep", None),
            P("pipe", None),
            P("pipe", "tp", None),
            P("pipe", "tp", None),
            P("pipe", None, "tp"),
            P("pipe", None, "tp"),
        ),
        out_specs=P("pipe", "rep", None, "tp"),
        check_vma=False,
    )
```

```python
import functools

import jax
import jax.numpy as jnp
from jax import lax
from jax.experimental import pallas as pl
from jax.experimental.pallas import tpu as pltpu
from jax.sharding import PartitionSpec as P

EPSILON = 1e-05


def shifted(x, axis, by):
    size = lax.axis_size(axis)
    pairs = [(i, i + by) for i in range(size) if 0 <= i + by < size]
    return lax.ppermute(x, axis, pairs)


def times_rows(left, weight):
    return lax.dot_general(
        left, weight, (((1,), (1,)), ((), ())), preferred_element_type=jnp.float32
    )


def block_step(
    current, unit_ids, unit_live, gain_full, up_weight, down_weight, shrink_weight, expand_weight
):
    row_count = current.shape[0]
    col_count = current.shape[1]
    hid_count = up_weight.shape[0]
    segments = unit_ids.shape[0]
    seg_rows = row_count // segments
    feature_width = gain_full.shape[0]
    adapter_rank_count = shrink_weight.shape[1] // col_count
    column = lax.axis_index("tp") * col_count
    gain_mine = lax.dynamic_slice_in_dim(gain_full, column, col_count, 0)
    widened_local = current.astype(jnp.float32)
    local_scaled = (widened_local * gain_mine).astype(jnp.bfloat16)
    input_panel = shrink_weight[unit_ids].reshape(segments, col_count, adapter_rank_count)
    output_panel = expand_weight[unit_ids].reshape(segments, hid_count, adapter_rank_count)
    partial_value = jnp.einsum(
        "sdr,spd->rsp",
        input_panel,
        local_scaled.reshape(segments, seg_rows, col_count),
        preferred_element_type=jnp.float32,
    ).reshape(adapter_rank_count, row_count)
    local_squares = jnp.sum(widened_local * widened_local, axis=1)
    reduced, squares = lax.psum((partial_value, local_squares), "tp")
    widened = lax.all_gather(current, "tp", axis=1, tiled=True).astype(jnp.float32)
    scaled = (widened * gain_full).astype(jnp.bfloat16)
    up_total = times_rows(scaled, up_weight)
    inverse = lax.rsqrt(squares / feature_width + EPSILON)
    low_rank = (
        (reduced * inverse[None, :])
        .astype(jnp.bfloat16)
        .reshape(adapter_rank_count, segments, seg_rows)
    )
    adapted = jnp.einsum(
        "rsp,sdr->spd", low_rank, output_panel, preferred_element_type=jnp.float32
    ).reshape(row_count, hid_count)
    up_sum = inverse[:, None] * up_total + adapted
    hidden_act = jax.nn.silu(up_sum).astype(jnp.bfloat16)
    down_sum = times_rows(lax.all_gather(hidden_act, "tp", axis=1, tiled=True), down_weight)
    updated = (widened_local + down_sum).astype(jnp.bfloat16)
    positions = lax.broadcasted_iota(jnp.int32, (segments, seg_rows), 1)
    row_kept = (positions < unit_live[:, None]).reshape(row_count, 1)
    return jnp.where(row_kept, updated, jnp.zeros_like(updated))


MESH = pl.DeviceIdType.MESH
PIECE = 256
COLUMNS = 2
LANES = 128
VMEM_BYTES = 67_043_328
NT = (((1,), (1,)), ((), ()))


class Spread:
    def __init__(self, buf, send, recv, pieces, z, x, depth, starts_own):
        self.buf, self.send, self.recv, self.pieces = buf, send, recv, pieces
        self.z, self.x, self.depth, self.starts_own = z, x, depth, starts_own
        self.shards = depth * COLUMNS
        self.me = z * COLUMNS + x

    def copy(self, t, c, way, target):
        return pltpu.make_async_remote_copy(
            src_ref=self.buf.at[t, c], dst_ref=self.buf.at[t, c],
            send_sem=self.send.at[way, t, c], recv_sem=self.recv.at[t, c],
            device_id={"tp": target}, device_id_type=MESH)

    def each(self, source_z, column, c, do):
        z, x, me = self.z, self.x, self.me
        t = source_z * COLUMNS + column
        own, special = column == x, c == self.pieces - 1
        along = jnp.logical_or(own, special)
        across = jnp.logical_and(own, jnp.logical_or(c != self.pieces - 1, source_z == z))

        @pl.when(jnp.logical_and(along, jnp.logical_and(source_z <= z, z < self.depth - 1)))
        def _():
            do(self.copy(t, c, 0, (me + COLUMNS) % self.shards))

        @pl.when(jnp.logical_and(along, jnp.logical_and(source_z >= z, z > 0)))
        def _():
            do(self.copy(t, c, 1, (me + self.shards - COLUMNS) % self.shards))

        @pl.when(across)
        def _():
            do(self.copy(t, c, 2, z * COLUMNS + (1 - x)))

    def forward(self, source_z, column, c):
        self.each(source_z, column, c, lambda d: d.start())

    def arrive(self, t, c):
        self.copy(t, c, 2, self.z * COLUMNS + (1 - self.x)).wait_recv()

    def relay(self, step, column, c):
        for source_z in (self.z - step, self.z + step) if step else (self.z,):
            @pl.when(jnp.logical_and(source_z >= 0, source_z < self.depth))
            def _():
                self.arrive(source_z * COLUMNS + column, c)
                self.forward(source_z, column, c)

    def drain(self):
        @pl.loop(0, self.depth)
        def _(source_z):
            @pl.when(jnp.logical_or(source_z != self.z, self.starts_own))
            def _():
                @pl.loop(0, self.pieces)
                def _(c):
                    self.each(source_z, self.x, c, lambda d: d.wait_send())

            self.each(source_z, 1 - self.x, self.pieces - 1, lambda d: d.wait_send())


def section_kernel(
    ids_ref, live_ref, gain_ref, x_hbm, reduce_hbm, expand_hbm, up_hbm, down_hbm, out_ref,
    up_v, down_v, xs, act, acc, sq, shrink, expand, partial,
    up_sem, down_sem, tab_sem, own_sem, part_send, part_recv, x_send, x_recv, a_send, a_recv, h_send,
):
    shards, x_pieces, rows, _ = xs.shape
    a_pieces = act.shape[1]
    cols = x_pieces * PIECE
    hidden = up_v.shape[0]
    width = shards * cols
    adapters, shrink_len = reduce_hbm.shape
    expand_len = expand_hbm.shape[1]
    segments = ids_ref.shape[0]
    rank = shrink_len // cols
    table_width = shards * hidden // (PIECE * rank) * (PIECE * rank)
    seg_rows = rows // segments
    depth = shards // COLUMNS
    me = lax.axis_index("tp")
    stage = lax.axis_index("pipe")
    stages = lax.axis_size("pipe")
    z, x = me // COLUMNS, me % COLUMNS
    partner = z * COLUMNS + (1 - x)
    upper = (me + COLUMNS) % shards
    lower = (me + shards - COLUMNS) % shards
    f32, bf16 = jnp.float32, jnp.bfloat16

    few = jnp.minimum(z, depth - 1 - z)
    layer = [z]
    for i in range(1, depth):
        both = i <= 2 * few
        far = jnp.where(both, (i + 1) // 2, i - few)
        down_side = jnp.where(both, i % 2 == 1, z > depth - 1 - z)
        layer.append(jnp.where(down_side, z - far, z + far))

    def shard(i, other):
        return layer[i] * COLUMNS + ((1 - x) if other else x)

    visits = [shard(i, other) for i in range(depth) for other in (False, True)]

    def up_copy(t):
        span = pl.ds(pl.multiple_of(t * cols, LANES), cols)
        return pltpu.make_async_copy(up_hbm.at[:, span], up_v.at[:, span], up_sem.at[t])

    def down_copy(t):
        span = pl.ds(pl.multiple_of(t * hidden, LANES), hidden)
        return pltpu.make_async_copy(down_hbm.at[:, span], down_v.at[:, span], down_sem.at[t])

    def own_copy(c):
        return pltpu.make_async_copy(x_hbm.at[:, c * PIECE:(c + 1) * PIECE], xs.at[me, c], own_sem.at[c])

    tables = []
    for table, length in ((reduce_hbm, shrink_len), (expand_hbm, expand_len)):
        blocks = []
        for at in range(0, length, table_width):
            size = min(table_width, length - at)
            k = sum(len(t) for t in tables) + len(blocks)
            copy = pltpu.make_async_copy(
                table.at[:, at:at + size],
                down_v.at[k * adapters:(k + 1) * adapters, 0:size], tab_sem.at[k])
            blocks.append((k, size, copy))
        tables.append(blocks)

    def start_tables(blocks):
        for _k, _size, copy in blocks:
            copy.start()

    def start_each(copy, order):
        for t in order:
            copy(t).start()

    @pl.when(stage == 0)
    def _():
        for c in range(x_pieces):
            own_copy(c).start()
        up_copy(me).start()

    @pl.when(stage > 0)
    def _():
        start_tables(tables[0])
        start_tables(tables[1])
        start_each(up_copy, visits)

    barrier = pltpu.get_barrier_semaphore()

    @pl.loop(1, shards)
    def _(i):
        pl.semaphore_signal(barrier, inc=1, device_id={"tp": (me + i) % shards}, device_id_type=MESH)

    def greet(target):
        pl.semaphore_signal(
            barrier, inc=1, device_id={"pipe": stage - 1, "tp": target}, device_id_type=MESH)

    @pl.when(stage > 0)
    def _():
        greet(me)
        greet(partner)

        @pl.when(z < depth - 1)
        def _():
            greet(upper)

        @pl.when(z > 0)
        def _():
            greet(lower)

    x_side = Spread(xs, x_send, x_recv, x_pieces, z, x, depth, stage == 0)
    a_side = Spread(act, a_send, a_recv, a_pieces, z, x, depth, stage >= 0)

    def hand_over(c, way, target):
        return pltpu.make_async_remote_copy(
            src_ref=out_ref.at[:, pl.ds(pl.multiple_of(c * PIECE, LANES), PIECE)], dst_ref=xs.at[me, c],
            send_sem=h_send.at[way, c], recv_sem=x_recv.at[me, c],
            device_id={"pipe": (stage + 1) % stages, "tp": target}, device_id_type=MESH)

    def hand_each(c, do):
        @pl.when(stage < stages - 1)
        def _():
            @pl.when(z < depth - 1)
            def _():
                do(hand_over(c, 0, upper))

            @pl.when(z > 0)
            def _():
                do(hand_over(c, 1, lower))

            do(hand_over(c, 2, partner))
            do(hand_over(c, 3, me))

    row_seg = lax.broadcasted_iota(jnp.int32, (rows, LANES), 0) // seg_rows
    lane_group = lax.broadcasted_iota(jnp.int32, (rows, LANES), 1) // rank
    in_segment = row_seg == lane_group

    picks = jnp.zeros((8 * segments, adapters), f32)
    pick_row = lax.broadcasted_iota(jnp.int32, picks.shape, 0)
    pick_col = lax.broadcasted_iota(jnp.int32, picks.shape, 1)
    for s in range(segments):
        hit = jnp.logical_and(pick_row // 8 == s, pick_col == ids_ref[s])
        picks = jnp.where(hit, 1.0, picks)
    picks = picks.astype(bf16)
    flat = PIECE * rank
    lane_tiles = flat // LANES
    spot_row = lax.broadcasted_iota(jnp.int32, (PIECE, LANES), 0) % 8
    spot_lane = lax.broadcasted_iota(jnp.int32, (PIECE, LANES), 1) // rank
    spot = spot_row == spot_lane
    fold_row = lax.broadcasted_iota(jnp.int32, (segments * LANES, LANES), 0)
    fold_col = lax.broadcasted_iota(jnp.int32, (segments * LANES, LANES), 1)
    fold = jnp.where(fold_col == fold_row // LANES * rank + fold_row % rank, 1.0, 0.0).astype(bf16)

    def panels(blocks, dest):
        done = 0
        for k, size, copy in blocks:
            copy.wait()
        for k, size, copy in blocks:
            first = done

            @pl.loop(0, size // flat)
            def _(j):
                span = pl.ds(pl.multiple_of(j * flat, LANES), flat)
                table = down_v[k * adapters:(k + 1) * adapters, span]
                got = jnp.dot(picks, table, preferred_element_type=f32)
                parts = []
                for s in range(segments):
                    tall = jnp.concatenate(
                        [got[8 * s:8 * s + 8, LANES * i:LANES * (i + 1)] for i in range(lane_tiles)], axis=0)
                    parts.append(jnp.where(spot, tall, 0.0).astype(bf16))
                panel = jnp.dot(jnp.concatenate(parts, axis=1), fold, preferred_element_type=f32)
                at = pl.multiple_of((first + j) * PIECE, PIECE)
                dest[pl.ds(at, PIECE), :] = panel.astype(bf16)

            done += size // flat

    def raw(t, c):
        return xs[t, c].astype(f32)

    def scaled(t, c, wide):
        at = pl.multiple_of(t * cols + c * PIECE, LANES)
        return (wide * gain_ref[:, pl.ds(at, PIECE)]).astype(bf16)

    def squares(wide):
        square = wide * wide
        return square[:, :LANES] + square[:, LANES:]

    def up_tile(n, t, c):
        at = pl.multiple_of(t * cols + c * PIECE, LANES)
        return up_v[n * PIECE:(n + 1) * PIECE, pl.ds(at, PIECE)]

    def up_add(items, init):
        lefts = []
        total = jnp.zeros((rows, LANES), f32) if init else sq[...]
        for t, c in items:
            wide = raw(t, c)
            total += squares(wide)
            lefts.append(scaled(t, c, wide))
        sq[...] = total
        for n in range(a_pieces):
            block = slice(n * PIECE, (n + 1) * PIECE)
            part = jnp.zeros((rows, PIECE), f32)
            for (t, c), left in zip(items, lefts):
                part += lax.dot_general(left, up_tile(n, t, c), NT, preferred_element_type=f32)
            acc[:, block] = part if init else acc[:, block] + part

    def own_up():
        up_add([(me, c) for c in range(x_pieces)], True)

    @pl.when(stage == 0)
    def _():
        for c in range(x_pieces):
            own_copy(c).wait()
        up_copy(me).wait()
        start_tables(tables[0])
        own_up()

    fed = 2 + jnp.where(z < depth - 1, 1, 0) + jnp.where(z > 0, 1, 0)
    pl.semaphore_wait(barrier, shards - 1 + jnp.where(stage < stages - 1, fed, 0))

    @pl.when(stage == 0)
    def _():
        for c in range(x_pieces):
            x_side.forward(z, x, c)
        start_each(up_copy, visits[1:3])
        panels(tables[0], shrink)

    @pl.when(stage > 0)
    def _():
        panels(tables[0], shrink)
        panels(tables[1], expand)
        start_each(down_copy, visits)

    @pl.when(stage > 0)
    def _():
        for c in range(x_pieces):
            x_side.arrive(me, c)
        up_copy(me).wait()
        own_up()

    def part_copy(owner, target):
        return pltpu.make_async_remote_copy(
            src_ref=partial.at[owner], dst_ref=partial.at[owner], send_sem=part_send.at[target],
            recv_sem=part_recv.at[owner], device_id={"tp": target}, device_id_type=MESH)

    def send_part():
        low = jnp.zeros((rows, LANES), f32)
        for c in range(x_pieces):
            low += jnp.dot(scaled(me, c, raw(me, c)), shrink[c * PIECE:(c + 1) * PIECE, :],
                           preferred_element_type=f32)
        low = jnp.where(in_segment, low, 0.0)
        if rows < LANES:
            low = jnp.concatenate([low, jnp.zeros((LANES - rows, LANES), f32)], axis=0)
        turned = jnp.transpose(low)
        picked = turned[0:rank]
        for s in range(1, segments):
            picked = picked + turned[s * rank:(s + 1) * rank]
        partial[me] = picked

        @pl.loop(1, shards)
        def _(i):
            part_copy(me, (me + i) % shards).start()

    def spread_in(side, step, weights, pieces_of, add, group):
        for t in weights:
            t.wait()

        @pl.loop(0, side.pieces // group)
        def _(j):
            for g in range(group):
                c = j * group + g
                side.relay(step, x, c)

                @pl.when(c < side.pieces - 1)
                def _():
                    side.arrive(shard(step - 1, True), c)

                @pl.when(c == side.pieces - 1)
                def _():
                    side.relay(step - 1, 1 - x, c)

            add([(t, j * group + g) for t in pieces_of for g in range(group)])

    send_part()

    for i in range(1, depth):
        fresh = [shard(i - 1, True), shard(i, False)]

        @pl.when(stage == 0)
        def _():
            if i == 1:
                start_tables(tables[1])
            if i == 2:
                start_each(up_copy, visits[6:])
            if i == depth - 1:
                start_each(down_copy, visits[:3])

        spread_in(x_side, i, [up_copy(t) for t in fresh], fresh, lambda items: up_add(items, False),
                  2 if x_pieces % 2 == 0 else 1)
        if i == 1:
            @pl.when(stage == 0)
            def _():
                start_each(up_copy, visits[3:6])
                panels(tables[1], expand)

    last = shard(depth - 1, True)
    up_copy(last).wait()
    for c in range(x_pieces - 2):
        x_side.arrive(last, c)
    up_add([(last, c) for c in range(x_pieces - 2)], False)

    @pl.loop(1, shards)
    def _(i):
        owner = (me + i) % shards
        part_copy(owner, owner).wait_recv()

    summed = partial[0]
    for t in range(1, shards):
        summed = summed + partial[t]
    stacked = jnp.concatenate([summed] * segments + [jnp.zeros((LANES - segments * rank, LANES), f32)], axis=0)
    low = jnp.where(in_segment, jnp.transpose(stacked)[:rows], 0.0)

    @pl.when(stage == 0)
    def _():
        start_each(down_copy, visits[3:5])

    x_side.arrive(last, x_pieces - 2)
    x_side.relay(depth - 1, 1 - x, x_pieces - 1)
    finals = [(last, x_pieces - 2), (last, x_pieces - 1)]
    square = sq[...]
    lefts = []
    for t, c in finals:
        wide = raw(t, c)
        square += squares(wide)
        lefts.append(scaled(t, c, wide))
    inverse = lax.rsqrt(jnp.sum(square, axis=1, keepdims=True) / width + EPSILON)
    low_rank = (low * inverse).astype(bf16)

    for n in range(a_pieces):
        block = slice(n * PIECE, (n + 1) * PIECE)
        base = jnp.zeros((rows, PIECE), f32)
        for (t, c), left in zip(finals, lefts):
            base += lax.dot_general(left, up_tile(n, t, c), NT, preferred_element_type=f32)
        adapted = lax.dot_general(low_rank, expand[block, :], NT, preferred_element_type=f32)
        value = inverse * (acc[:, block] + base) + adapted
        act[me, n] = (value / (1.0 + jnp.exp(-value))).astype(bf16)
        a_side.forward(z, x, n)

    def down_tile(n, t, c):
        at = pl.multiple_of(t * hidden + c * PIECE, LANES)
        return down_v[n * PIECE:(n + 1) * PIECE, pl.ds(at, PIECE)]

    def down_add(items):
        for n in range(x_pieces):
            block = slice(n * PIECE, (n + 1) * PIECE)
            part = jnp.zeros((rows, PIECE), f32)
            for t, c in items:
                part += lax.dot_general(act[t, c], down_tile(n, t, c), NT, preferred_element_type=f32)
            acc[:, block] = acc[:, block] + part

    @pl.when(stage == 0)
    def _():
        start_each(down_copy, visits[5:])

    for n in range(x_pieces):
        acc[:, n * PIECE:(n + 1) * PIECE] = xs[me, n].astype(f32)

    down_copy(me).wait()
    for i in range(1, depth):
        fresh = [shard(i - 1, True), shard(i, False)]
        spread_in(a_side, i, [down_copy(t) for t in fresh],
                  ([me] if i == 1 else []) + fresh, down_add, 1)

    down_copy(last).wait()

    @pl.loop(0, a_pieces - 2)
    def _(c):
        a_side.arrive(last, c)
        down_add([(last, c)])

    row = lax.broadcasted_iota(jnp.int32, (rows, 1), 0)
    kept = row < 0
    for s in range(segments):
        start = s * seg_rows
        kept = jnp.logical_or(kept, jnp.logical_and(row >= start, row < start + jnp.minimum(live_ref[s], seg_rows)))

    a_side.arrive(last, a_pieces - 2)
    a_side.relay(depth - 1, 1 - x, a_pieces - 1)
    for n in range(x_pieces):
        block = slice(n * PIECE, (n + 1) * PIECE)
        part = jnp.zeros((rows, PIECE), f32)
        for c in (a_pieces - 2, a_pieces - 1):
            part += lax.dot_general(act[last, c], down_tile(n, last, c), NT, preferred_element_type=f32)
        out_ref[:, block] = jnp.where(kept, acc[:, block] + part, 0.0).astype(bf16)
        hand_each(n, lambda d: d.start())

    @pl.loop(0, x_pieces)
    def _(c):
        hand_each(c, lambda d: d.wait_send())

    @pl.loop(1, shards)
    def _(i):
        part_copy(me, (me + i) % shards).wait_send()

    x_side.drain()
    a_side.drain()


def fused_sections(current, ids, live, gain, up_weight, down_weight, shrink_weight, expand_weight):
    rows, cols = current.shape
    hidden = up_weight.shape[0]
    shards = lax.axis_size("tp")
    rank = shrink_weight.shape[1] // cols
    x_pieces, a_pieces = cols // PIECE, hidden // PIECE
    vmem = pl.BlockSpec(memory_space=pltpu.VMEM)
    smem = pl.BlockSpec(memory_space=pltpu.SMEM)
    hbm = pl.BlockSpec(memory_space=pl.ANY)
    dma = pltpu.SemaphoreType.DMA
    flat = PIECE * rank
    blocks = table_blocks(shards * hidden // flat * flat, shrink_weight, expand_weight)
    return pl.pallas_call(
        section_kernel,
        out_shape=jax.ShapeDtypeStruct((rows, cols), jnp.bfloat16),
        in_specs=[smem, smem, vmem] + [hbm] * 5,
        out_specs=vmem,
        scratch_shapes=[
            pltpu.VMEM(up_weight.shape, jnp.bfloat16),
            pltpu.VMEM(down_weight.shape, jnp.bfloat16),
            pltpu.VMEM((shards, x_pieces, rows, PIECE), jnp.bfloat16),
            pltpu.VMEM((shards, a_pieces, rows, PIECE), jnp.bfloat16),
            pltpu.VMEM((rows, hidden), jnp.float32),
            pltpu.VMEM((rows, LANES), jnp.float32),
            pltpu.VMEM((cols, LANES), jnp.bfloat16),
            pltpu.VMEM((hidden, LANES), jnp.bfloat16),
            pltpu.VMEM((shards, rank, LANES), jnp.float32),
            dma((shards,)), dma((shards,)), dma((blocks,)), dma((x_pieces,)),
            dma((shards,)), dma((shards,)),
            dma((3, shards, x_pieces)), dma((shards, x_pieces)),
            dma((3, shards, a_pieces)), dma((shards, a_pieces)),
            dma((4, x_pieces)),
        ],
        compiler_params=pltpu.CompilerParams(
            collective_id=0, has_side_effects=True, vmem_limit_bytes=VMEM_BYTES
        ),
    )(ids, live, gain[None, :], current, shrink_weight, expand_weight, up_weight, down_weight)


def table_blocks(width, *tables):
    return sum(-(-table.shape[1] // width) for table in tables)


def kernel_fits(row_count, col_count, hidden, segments, shrink_weight, expand_weight):
    shards = lax.axis_size("tp")
    adapters, flat_cols = shrink_weight.shape
    rank = flat_cols // col_count
    flat = PIECE * rank
    width = shards * hidden // flat * flat
    if col_count % PIECE or hidden % PIECE or hidden < 4 * PIECE or col_count < 4 * PIECE:
        return False
    if row_count > LANES or rank * 8 != LANES or segments * rank > LANES or adapters % LANES:
        return False
    if shards % COLUMNS or shards < 2 * COLUMNS or col_count > hidden:
        return False
    if not width or table_blocks(width, shrink_weight, expand_weight) * adapters > col_count:
        return False
    return 2 * hidden * col_count * 2 * shards < VMEM_BYTES - 7 * 2**20


def run_window(
    units, unit_ids, unit_live, gain_full, up_weight, down_weight, shrink_weight, expand_weight
):
    section_index = lax.axis_index("pipe")
    sections = lax.axis_size("pipe")
    unit_count = units.shape[0]
    tick_total = unit_count + sections - 1

    def process(tick_index, received, collected):
        position = jnp.clip(tick_index - section_index, 0, unit_count - 1)
        arriving = lax.dynamic_index_in_dim(
            units, jnp.minimum(tick_index, unit_count - 1), 0, keepdims=False
        )
        current = jnp.where(section_index == 0, arriving, received)
        ids_here = lax.dynamic_index_in_dim(unit_ids, position, 0, keepdims=False)
        live_here = lax.dynamic_index_in_dim(unit_live, position, 0, keepdims=False)
        produced = block_step(
            current,
            ids_here,
            live_here,
            gain_full,
            up_weight,
            down_weight,
            shrink_weight,
            expand_weight,
        )
        lag = tick_index - section_index
        in_window = jnp.logical_and(lag >= 0, lag < unit_count)
        placed = lax.dynamic_update_index_in_dim(collected, produced, position, 0)
        return (produced, jnp.where(in_window, placed, collected))

    def one_tick(tick_index, state):
        produced, collected = process(tick_index, state[0], state[1])
        return (shifted(produced, "pipe", 1), collected)

    start_state = (jnp.zeros_like(units[0]), jnp.zeros_like(units))
    received, collected = lax.fori_loop(0, tick_total - 1, one_tick, start_state)
    produced, collected = process(tick_total - 1, received, collected)
    return collected


def per_device(
    hidden_entering,
    segment_adapter,
    segment_requests,
    section_norm_gain,
    up_matrix,
    down_matrix,
    adapter_reduce,
    adapter_expand,
):
    batch_list = hidden_entering.shape[0]
    row_count = hidden_entering.shape[1]
    col_count = hidden_entering.shape[2]
    hidden = up_matrix.shape[1]
    segments = segment_adapter.shape[1]
    if batch_list == 1 and kernel_fits(
        row_count, col_count, hidden, segments, adapter_reduce[0], adapter_expand[0]
    ):
        produced = fused_sections(
            hidden_entering[0],
            segment_adapter[0],
            segment_requests[0],
            section_norm_gain[0],
            up_matrix[0],
            down_matrix[0],
            adapter_reduce[0],
            adapter_expand[0],
        )
        return produced.reshape(1, batch_list, row_count, col_count)
    collected = run_window(
        hidden_entering,
        segment_adapter,
        segment_requests,
        section_norm_gain[0],
        up_matrix[0],
        down_matrix[0],
        adapter_reduce[0],
        adapter_expand[0],
    )
    return collected.reshape(1, batch_list, row_count, col_count)


def solution(mesh):
    return jax.shard_map(
        per_device,
        mesh=mesh,
        in_specs=(
            P("rep", None, "tp"),
            P("rep", None),
            P("rep", None),
            P("pipe", None),
            P("pipe", "tp", None),
            P("pipe", "tp", None),
            P("pipe", None, "tp"),
            P("pipe", None, "tp"),
        ),
        out_specs=P("pipe", "rep", None, "tp"),
        check_vma=False,
    )
```

```python
import functools

import jax
import jax.numpy as jnp
from jax import lax
from jax.experimental import pallas as pl
from jax.experimental.pallas import tpu as pltpu
from jax.sharding import PartitionSpec as P

EPSILON = 1e-05


def shifted(x, axis, by):
    size = lax.axis_size(axis)
    pairs = [(i, i + by) for i in range(size) if 0 <= i + by < size]
    return lax.ppermute(x, axis, pairs)


def times_rows(left, weight):
    return lax.dot_general(
        left, weight, (((1,), (1,)), ((), ())), preferred_element_type=jnp.float32
    )


def block_step(
    current, unit_ids, unit_live, gain_full, up_weight, down_weight, shrink_weight, expand_weight
):
    row_count = current.shape[0]
    col_count = current.shape[1]
    hid_count = up_weight.shape[0]
    segments = unit_ids.shape[0]
    seg_rows = row_count // segments
    feature_width = gain_full.shape[0]
    adapter_rank_count = shrink_weight.shape[1] // col_count
    column = lax.axis_index("tp") * col_count
    gain_mine = lax.dynamic_slice_in_dim(gain_full, column, col_count, 0)
    widened_local = current.astype(jnp.float32)
    local_scaled = (widened_local * gain_mine).astype(jnp.bfloat16)
    input_panel = shrink_weight[unit_ids].reshape(segments, col_count, adapter_rank_count)
    output_panel = expand_weight[unit_ids].reshape(segments, hid_count, adapter_rank_count)
    partial_value = jnp.einsum(
        "sdr,spd->rsp",
        input_panel,
        local_scaled.reshape(segments, seg_rows, col_count),
        preferred_element_type=jnp.float32,
    ).reshape(adapter_rank_count, row_count)
    local_squares = jnp.sum(widened_local * widened_local, axis=1)
    reduced, squares = lax.psum((partial_value, local_squares), "tp")
    widened = lax.all_gather(current, "tp", axis=1, tiled=True).astype(jnp.float32)
    scaled = (widened * gain_full).astype(jnp.bfloat16)
    up_total = times_rows(scaled, up_weight)
    inverse = lax.rsqrt(squares / feature_width + EPSILON)
    low_rank = (
        (reduced * inverse[None, :])
        .astype(jnp.bfloat16)
        .reshape(adapter_rank_count, segments, seg_rows)
    )
    adapted = jnp.einsum(
        "rsp,sdr->spd", low_rank, output_panel, preferred_element_type=jnp.float32
    ).reshape(row_count, hid_count)
    up_sum = inverse[:, None] * up_total + adapted
    hidden_act = jax.nn.silu(up_sum).astype(jnp.bfloat16)
    down_sum = times_rows(lax.all_gather(hidden_act, "tp", axis=1, tiled=True), down_weight)
    updated = (widened_local + down_sum).astype(jnp.bfloat16)
    positions = lax.broadcasted_iota(jnp.int32, (segments, seg_rows), 1)
    row_kept = (positions < unit_live[:, None]).reshape(row_count, 1)
    return jnp.where(row_kept, updated, jnp.zeros_like(updated))


MESH = pl.DeviceIdType.MESH
PIECE = 256
COLUMNS = 2
LANES = 128
VMEM_BYTES = 67_043_328
NT = (((1,), (1,)), ((), ()))


class Spread:
    OWN, ALONG, EXTRA, ACROSS = range(4)

    def __init__(self, buf, send, recv, pieces, z, x, depth, starts_own):
        self.buf, self.send, self.recv, self.pieces = buf, send, recv, pieces
        self.z, self.x, self.depth, self.starts_own = z, x, depth, starts_own
        self.shards = depth * COLUMNS
        self.me = z * COLUMNS + x

    def copy(self, t, c, kind, target):
        return pltpu.make_async_remote_copy(
            src_ref=self.buf.at[t, c], dst_ref=self.buf.at[t, c],
            send_sem=self.send.at[kind], recv_sem=self.recv.at[t, c],
            device_id={"tp": target}, device_id_type=MESH)

    def start_along(self, source_z, t, c, kind):
        z, me = self.z, self.me

        @pl.when(jnp.logical_and(source_z <= z, z < self.depth - 1))
        def _():
            self.copy(t, c, kind, (me + COLUMNS) % self.shards).start()

        @pl.when(jnp.logical_and(source_z >= z, z > 0))
        def _():
            self.copy(t, c, kind, (me + self.shards - COLUMNS) % self.shards).start()

    def start_across(self, t, c, kind):
        self.copy(t, c, kind, self.z * COLUMNS + (1 - self.x)).start()

    def start_own(self, c):
        self.start_along(self.z, self.me, c, self.OWN)
        self.start_across(self.me, c, self.OWN)

    def arrive(self, t, c):
        self.copy(t, c, self.ACROSS, self.z * COLUMNS + (1 - self.x)).wait_recv()

    def both_sides(self, step, do):
        for source_z in (self.z - step, self.z + step) if step else (self.z,):
            @pl.when(jnp.logical_and(source_z >= 0, source_z < self.depth))
            def _():
                do(source_z)

    def relay(self, step, c):
        def do(source_z):
            t = source_z * COLUMNS + self.x
            self.arrive(t, c)
            self.start_along(source_z, t, c, self.ALONG)

            @pl.when(c < self.pieces - 1)
            def _():
                self.start_across(t, c, self.ACROSS)

        self.both_sides(step, do)

    def relay_extra(self, step):
        def do(source_z):
            t = source_z * COLUMNS + 1 - self.x
            self.arrive(t, self.pieces - 1)
            self.start_along(source_z, t, self.pieces - 1, self.EXTRA)

        self.both_sides(step, do)

    def sent(self, kind, outer, inner, filler):
        if outer and inner:
            view = filler.at[0:outer, 0:inner]
            pltpu.make_async_remote_copy(
                src_ref=view, dst_ref=view, send_sem=self.send.at[kind], recv_sem=self.recv.at[0, 0],
                device_id={"tp": self.me}, device_id_type=MESH).wait_send()

    def drain(self, filler):
        for z in range(self.depth):
            ways = (z < self.depth - 1) + (z > 0)
            layers = (z + 1) * (z < self.depth - 1) + (self.depth - z) * (z > 0)

            @pl.when(self.z == z)
            def _():
                @pl.when(self.starts_own)
                def _():
                    self.sent(self.OWN, ways + 1, self.pieces, filler)

                self.sent(self.ALONG, layers - ways, self.pieces, filler)
                self.sent(self.EXTRA, layers, 1, filler)

        self.sent(self.ACROSS, self.depth - 1, self.pieces - 1, filler)


def section_kernel(
    ids_ref, live_ref, gain_ref, x_hbm, reduce_hbm, expand_hbm, up_hbm, down_hbm, out_hbm,
    up_v, down_v, xs, act, acc, sq, shrink, expand, partial, out_v,
    up_sem, down_sem, tab_sem, own_sem, part_send, part_recv, x_send, x_recv, a_send, a_recv, h_send, out_sem,
):
    shards, x_pieces, rows, _ = xs.shape
    a_pieces = act.shape[1]
    cols = x_pieces * PIECE
    hidden = up_v.shape[0]
    width = shards * cols
    adapters, shrink_len = reduce_hbm.shape
    expand_len = expand_hbm.shape[1]
    segments = ids_ref.shape[0]
    rank = shrink_len // cols
    table_width = shards * hidden // (PIECE * rank) * (PIECE * rank)
    seg_rows = rows // segments
    depth = shards // COLUMNS
    me = lax.axis_index("tp")
    stage = lax.axis_index("pipe")
    stages = lax.axis_size("pipe")
    z, x = me // COLUMNS, me % COLUMNS
    partner = z * COLUMNS + (1 - x)
    upper = (me + COLUMNS) % shards
    lower = (me + shards - COLUMNS) % shards
    f32, bf16 = jnp.float32, jnp.bfloat16

    few = jnp.minimum(z, depth - 1 - z)
    layer = [z]
    for i in range(1, depth):
        both = i <= 2 * few
        far = jnp.where(both, (i + 1) // 2, i - few)
        down_side = jnp.where(both, i % 2 == 1, z > depth - 1 - z)
        layer.append(jnp.where(down_side, z - far, z + far))

    def shard(i, other):
        return layer[i] * COLUMNS + ((1 - x) if other else x)

    visits = [shard(i, other) for i in range(depth) for other in (False, True)]

    def up_copy(t):
        span = pl.ds(pl.multiple_of(t * cols, LANES), cols)
        return pltpu.make_async_copy(up_hbm.at[:, span], up_v.at[:, span], up_sem.at[t])

    def down_copy(t):
        span = pl.ds(pl.multiple_of(t * hidden, LANES), hidden)
        return pltpu.make_async_copy(down_hbm.at[:, span], down_v.at[:, span], down_sem.at[t])

    def own_copy(c):
        return pltpu.make_async_copy(x_hbm.at[:, c * PIECE:(c + 1) * PIECE], xs.at[me, c], own_sem.at[0])

    tables = []
    for table, length in ((reduce_hbm, shrink_len), (expand_hbm, expand_len)):
        blocks = []
        for at in range(0, length, table_width):
            size = min(table_width, length - at)
            k = sum(len(t) for t in tables) + len(blocks)
            copy = pltpu.make_async_copy(
                table.at[:, at:at + size],
                down_v.at[k * adapters:(k + 1) * adapters, 0:size], tab_sem.at[k])
            blocks.append((k, size, copy))
        tables.append(blocks)

    def start_tables(blocks):
        for _k, _size, copy in blocks:
            copy.start()

    def start_each(copy, order):
        for t in order:
            copy(t).start()

    @pl.when(stage == 0)
    def _():
        for c in range(x_pieces):
            own_copy(c).start()
        up_copy(me).start()

    @pl.when(stage > 0)
    def _():
        start_tables(tables[0])
        start_tables(tables[1])
        start_each(up_copy, visits)

    barrier = pltpu.get_barrier_semaphore()

    @pl.loop(1, shards)
    def _(i):
        pl.semaphore_signal(barrier, inc=1, device_id={"tp": (me + i) % shards}, device_id_type=MESH)

    def greet(target):
        pl.semaphore_signal(
            barrier, inc=1, device_id={"pipe": stage - 1, "tp": target}, device_id_type=MESH)

    @pl.when(stage > 0)
    def _():
        greet(me)
        greet(partner)

        @pl.when(z < depth - 1)
        def _():
            greet(upper)

        @pl.when(z > 0)
        def _():
            greet(lower)

    x_side = Spread(xs, x_send, x_recv, x_pieces, z, x, depth, stage == 0)
    a_side = Spread(act, a_send, a_recv, a_pieces, z, x, depth, stage >= 0)

    def hand_over(c, target):
        return pltpu.make_async_remote_copy(
            src_ref=out_v.at[c], dst_ref=xs.at[me, c], send_sem=h_send.at[0], recv_sem=x_recv.at[me, c],
            device_id={"pipe": (stage + 1) % stages, "tp": target}, device_id_type=MESH)

    def hand_each(c):
        @pl.when(stage < stages - 1)
        def _():
            @pl.when(z < depth - 1)
            def _():
                hand_over(c, upper).start()

            @pl.when(z > 0)
            def _():
                hand_over(c, lower).start()

            hand_over(c, partner).start()
            hand_over(c, me).start()

    def hand_drain():
        for at in range(depth):
            count = 2 + (at < depth - 1) + (at > 0)

            @pl.when(jnp.logical_and(stage < stages - 1, z == at))
            def _():
                view = xs.at[0:count]
                pltpu.make_async_remote_copy(
                    src_ref=view, dst_ref=view, send_sem=h_send.at[0], recv_sem=x_recv.at[0, 0],
                    device_id={"tp": me}, device_id_type=MESH).wait_send()

    def out_copy(c):
        return pltpu.make_async_copy(out_v.at[c], out_hbm.at[:, c * PIECE:(c + 1) * PIECE], out_sem.at[0])

    row_seg = lax.broadcasted_iota(jnp.int32, (rows, LANES), 0) // seg_rows
    lane_group = lax.broadcasted_iota(jnp.int32, (rows, LANES), 1) // rank
    in_segment = row_seg == lane_group

    picks = jnp.zeros((8 * segments, adapters), f32)
    pick_row = lax.broadcasted_iota(jnp.int32, picks.shape, 0)
    pick_col = lax.broadcasted_iota(jnp.int32, picks.shape, 1)
    for s in range(segments):
        hit = jnp.logical_and(pick_row // 8 == s, pick_col == ids_ref[s])
        picks = jnp.where(hit, 1.0, picks)
    picks = picks.astype(bf16)
    flat = PIECE * rank
    lane_tiles = flat // LANES
    spot_row = lax.broadcasted_iota(jnp.int32, (PIECE, LANES), 0) % 8
    spot_lane = lax.broadcasted_iota(jnp.int32, (PIECE, LANES), 1) // rank
    spot = spot_row == spot_lane
    fold_row = lax.broadcasted_iota(jnp.int32, (segments * LANES, LANES), 0)
    fold_col = lax.broadcasted_iota(jnp.int32, (segments * LANES, LANES), 1)
    fold = jnp.where(fold_col == fold_row // LANES * rank + fold_row % rank, 1.0, 0.0).astype(bf16)

    def panels(blocks, dest):
        done = 0
        for k, size, copy in blocks:
            copy.wait()
        for k, size, copy in blocks:
            first = done

            @pl.loop(0, size // flat)
            def _(j):
                span = pl.ds(pl.multiple_of(j * flat, LANES), flat)
                table = down_v[k * adapters:(k + 1) * adapters, span]
                got = jnp.dot(picks, table, preferred_element_type=f32)
                parts = []
                for s in range(segments):
                    tall = jnp.concatenate(
                        [got[8 * s:8 * s + 8, LANES * i:LANES * (i + 1)] for i in range(lane_tiles)], axis=0)
                    parts.append(jnp.where(spot, tall, 0.0).astype(bf16))
                panel = jnp.dot(jnp.concatenate(parts, axis=1), fold, preferred_element_type=f32)
                at = pl.multiple_of((first + j) * PIECE, PIECE)
                dest[pl.ds(at, PIECE), :] = panel.astype(bf16)

            done += size // flat

    def raw(t, c):
        return xs[t, c].astype(f32)

    def scaled(t, c, wide):
        at = pl.multiple_of(t * cols + c * PIECE, LANES)
        return (wide * gain_ref[:, pl.ds(at, PIECE)]).astype(bf16)

    def squares(wide):
        square = wide * wide
        return square[:, :LANES] + square[:, LANES:]

    def up_tile(n, t, c):
        at = pl.multiple_of(t * cols + c * PIECE, LANES)
        return up_v[n * PIECE:(n + 1) * PIECE, pl.ds(at, PIECE)]

    def up_dot(left, n, t, c, flipped):
        dims = (((1,), (0,)), ((), ())) if flipped else NT
        return lax.dot_general(left, up_tile(n, t, c), dims, preferred_element_type=f32)

    def up_add(items, init, flipped):
        lefts = []
        total = jnp.zeros((rows, LANES), f32) if init else sq[...]
        for t, c in items:
            wide = raw(t, c)
            total += squares(wide)
            lefts.append(scaled(t, c, wide))
        sq[...] = total
        for n in range(a_pieces):
            block = slice(n * PIECE, (n + 1) * PIECE)
            part = jnp.zeros((rows, PIECE), f32)
            for (t, c), left in zip(items, lefts):
                part += up_dot(left, n, t, c, flipped)
            acc[:, block] = part if init else acc[:, block] + part

    def per_stage(work):
        @pl.when(stage == 0)
        def _():
            work(False)

        @pl.when(stage > 0)
        def _():
            work(True)

    def own_up(flipped):
        up_add([(me, c) for c in range(x_pieces)], True, flipped)

    def flip_up():
        for t in visits:
            up_copy(t).wait()

        @pl.loop(0, a_pieces * shards * x_pieces)
        def _(i):
            tall = pl.ds(pl.multiple_of(i // (shards * x_pieces) * PIECE, PIECE), PIECE)
            wide = pl.ds(pl.multiple_of(i % (shards * x_pieces) * PIECE, PIECE), PIECE)
            up_v[tall, wide] = jnp.transpose(up_v[tall, wide])

    def part_copy(owner, target):
        return pltpu.make_async_remote_copy(
            src_ref=partial.at[owner], dst_ref=partial.at[owner], send_sem=part_send.at[0],
            recv_sem=part_recv.at[0], device_id={"tp": target}, device_id_type=MESH)

    def send_part():
        low = jnp.zeros((rows, LANES), f32)
        for c in range(x_pieces):
            low += jnp.dot(scaled(me, c, raw(me, c)), shrink[c * PIECE:(c + 1) * PIECE, :],
                           preferred_element_type=f32)
        low = jnp.where(in_segment, low, 0.0)
        if rows < LANES:
            low = jnp.concatenate([low, jnp.zeros((LANES - rows, LANES), f32)], axis=0)
        turned = jnp.transpose(low)
        picked = turned[0:rank]
        for s in range(1, segments):
            picked = picked + turned[s * rank:(s + 1) * rank]
        partial[me] = picked

        @pl.loop(1, shards)
        def _(i):
            part_copy(me, (me + i) % shards).start()

    @pl.when(stage == 0)
    def _():
        pltpu.make_async_copy(xs.at[me], xs.at[me], own_sem.at[0]).wait()
        up_copy(me).wait()
        start_tables(tables[0])
        own_up(False)
        start_each(up_copy, visits[1:3])

    fed = 2 + jnp.where(z < depth - 1, 1, 0) + jnp.where(z > 0, 1, 0)
    pl.semaphore_wait(barrier, shards - 1 + jnp.where(stage < stages - 1, fed, 0))

    @pl.when(stage == 0)
    def _():
        for c in range(x_pieces):
            x_side.start_own(c)
        panels(tables[0], shrink)
        send_part()

    @pl.when(stage > 0)
    def _():
        panels(tables[0], shrink)
        panels(tables[1], expand)
        start_each(down_copy, visits)
        flip_up()

    @pl.when(stage > 0)
    def _():
        for c in range(x_pieces):
            x_side.arrive(me, c)
        own_up(True)

    def spread_in(side, step, pieces_of, add, group):
        @pl.loop(0, side.pieces // group)
        def _(j):
            for g in range(group):
                c = j * group + g
                side.relay(step, c)

                @pl.when(c < side.pieces - 1)
                def _():
                    side.arrive(shard(step - 1, True), c)

                @pl.when(c == side.pieces - 1)
                def _():
                    side.relay_extra(step - 1)

            add([(t, j * group + g) for t in pieces_of for g in range(group)])

    for i in range(1, depth):
        fresh = [shard(i - 1, True), shard(i, False)]

        @pl.when(stage == 0)
        def _():
            for t in fresh:
                up_copy(t).wait()
            if i == 1:
                start_tables(tables[1])
            if i == 2:
                start_each(up_copy, visits[6:])
            if i == depth - 1:
                start_each(down_copy, visits[:3])

        spread_in(x_side, i, fresh, lambda items: per_stage(functools.partial(up_add, items, False)), 2 if x_pieces % 2 == 0 else 1)
        if i == 1:
            @pl.when(stage == 0)
            def _():
                start_each(up_copy, visits[3:6])
                panels(tables[1], expand)

            @pl.when(stage > 0)
            def _():
                send_part()

    last = shard(depth - 1, True)

    @pl.when(stage == 0)
    def _():
        up_copy(last).wait()

    for c in range(x_pieces - 2):
        x_side.arrive(last, c)
    per_stage(functools.partial(up_add, [(last, c) for c in range(x_pieces - 2)], False))

    others = partial.at[0:shards - 1]
    all_parts = pltpu.make_async_remote_copy(
        src_ref=others, dst_ref=others, send_sem=part_send.at[0], recv_sem=part_recv.at[0],
        device_id={"tp": me}, device_id_type=MESH)
    all_parts.wait_recv()

    summed = partial[0]
    for t in range(1, shards):
        summed = summed + partial[t]
    stacked = jnp.concatenate([summed] * segments + [jnp.zeros((LANES - segments * rank, LANES), f32)], axis=0)
    low = jnp.where(in_segment, jnp.transpose(stacked)[:rows], 0.0)

    @pl.when(stage == 0)
    def _():
        start_each(down_copy, visits[3:5])

    x_side.arrive(last, x_pieces - 2)
    x_side.relay_extra(depth - 1)
    finals = [(last, x_pieces - 2), (last, x_pieces - 1)]
    square = sq[...]
    lefts = []
    for t, c in finals:
        wide = raw(t, c)
        square += squares(wide)
        lefts.append(scaled(t, c, wide))
    inverse = lax.rsqrt(jnp.sum(square, axis=1, keepdims=True) / width + EPSILON)
    low_rank = (low * inverse).astype(bf16)

    def up_finish(flipped):
        for n in range(a_pieces):
            block = slice(n * PIECE, (n + 1) * PIECE)
            base = jnp.zeros((rows, PIECE), f32)
            for (t, c), left in zip(finals, lefts):
                base += up_dot(left, n, t, c, flipped)
            adapted = lax.dot_general(low_rank, expand[block, :], NT, preferred_element_type=f32)
            value = inverse * (acc[:, block] + base) + adapted
            act[me, n] = (value / (1.0 + jnp.exp(-value))).astype(bf16)
            a_side.start_own(n)

    per_stage(up_finish)

    def down_tile(n, t, c):
        at = pl.multiple_of(t * hidden + c * PIECE, LANES)
        return down_v[n * PIECE:(n + 1) * PIECE, pl.ds(at, PIECE)]

    def down_add(items):
        for n in range(x_pieces):
            block = slice(n * PIECE, (n + 1) * PIECE)
            part = jnp.zeros((rows, PIECE), f32)
            for t, c in items:
                part += lax.dot_general(act[t, c], down_tile(n, t, c), NT, preferred_element_type=f32)
            acc[:, block] = acc[:, block] + part

    @pl.when(stage == 0)
    def _():
        start_each(down_copy, visits[5:])

    for n in range(x_pieces):
        acc[:, n * PIECE:(n + 1) * PIECE] = xs[me, n].astype(f32)

    down_copy(me).wait()
    for i in range(1, depth):
        fresh = [shard(i - 1, True), shard(i, False)]
        for t in fresh:
            down_copy(t).wait()
        spread_in(a_side, i, ([me] if i == 1 else []) + fresh, down_add, 1)

    down_copy(last).wait()

    @pl.loop(0, a_pieces - 2)
    def _(c):
        a_side.arrive(last, c)
        down_add([(last, c)])

    row = lax.broadcasted_iota(jnp.int32, (rows, 1), 0)
    kept = row < 0
    for s in range(segments):
        start = s * seg_rows
        kept = jnp.logical_or(kept, jnp.logical_and(row >= start, row < start + jnp.minimum(live_ref[s], seg_rows)))

    a_side.arrive(last, a_pieces - 2)
    a_side.relay_extra(depth - 1)
    for n in range(x_pieces):
        block = slice(n * PIECE, (n + 1) * PIECE)
        part = jnp.zeros((rows, PIECE), f32)
        for c in (a_pieces - 2, a_pieces - 1):
            part += lax.dot_general(act[last, c], down_tile(n, last, c), NT, preferred_element_type=f32)
        out_v[n] = jnp.where(kept, acc[:, block] + part, 0.0).astype(bf16)
        hand_each(n)
        out_copy(n).start()

    all_parts.wait_send()
    x_side.drain(act)
    a_side.drain(act)
    hand_drain()
    pltpu.make_async_copy(out_v, out_v, out_sem.at[0]).wait()


def fused_sections(current, ids, live, gain, up_weight, down_weight, shrink_weight, expand_weight):
    rows, cols = current.shape
    hidden = up_weight.shape[0]
    shards = lax.axis_size("tp")
    rank = shrink_weight.shape[1] // cols
    x_pieces, a_pieces = cols // PIECE, hidden // PIECE
    vmem = pl.BlockSpec(memory_space=pltpu.VMEM)
    smem = pl.BlockSpec(memory_space=pltpu.SMEM)
    hbm = pl.BlockSpec(memory_space=pl.ANY)
    dma = pltpu.SemaphoreType.DMA
    flat = PIECE * rank
    blocks = table_blocks(shards * hidden // flat * flat, shrink_weight, expand_weight)
    return pl.pallas_call(
        section_kernel,
        out_shape=jax.ShapeDtypeStruct((rows, cols), jnp.bfloat16),
        in_specs=[smem, smem, vmem] + [hbm] * 5,
        out_specs=hbm,
        scratch_shapes=[
            pltpu.VMEM(up_weight.shape, jnp.bfloat16),
            pltpu.VMEM(down_weight.shape, jnp.bfloat16),
            pltpu.VMEM((shards, x_pieces, rows, PIECE), jnp.bfloat16),
            pltpu.VMEM((shards, a_pieces, rows, PIECE), jnp.bfloat16),
            pltpu.VMEM((rows, hidden), jnp.float32),
            pltpu.VMEM((rows, LANES), jnp.float32),
            pltpu.VMEM((cols, LANES), jnp.bfloat16),
            pltpu.VMEM((hidden, LANES), jnp.bfloat16),
            pltpu.VMEM((shards, rank, LANES), jnp.float32),
            pltpu.VMEM((x_pieces, rows, PIECE), jnp.bfloat16),
            dma((shards,)), dma((shards,)), dma((blocks,)), dma((1,)),
            dma((1,)), dma((1,)),
            dma((4,)), dma((shards, x_pieces)),
            dma((4,)), dma((shards, a_pieces)),
            dma((1,)), dma((1,)),
        ],
        compiler_params=pltpu.CompilerParams(
            collective_id=0, has_side_effects=True, vmem_limit_bytes=VMEM_BYTES
        ),
    )(ids, live, gain[None, :], current, shrink_weight, expand_weight, up_weight, down_weight)


def table_blocks(width, *tables):
    return sum(-(-table.shape[1] // width) for table in tables)


def kernel_fits(row_count, col_count, hidden, segments, shrink_weight, expand_weight):
    shards = lax.axis_size("tp")
    adapters, flat_cols = shrink_weight.shape
    rank = flat_cols // col_count
    flat = PIECE * rank
    width = shards * hidden // flat * flat
    if col_count % PIECE or hidden % PIECE or hidden < 4 * PIECE or col_count < 4 * PIECE:
        return False
    if row_count > LANES or rank * 8 != LANES or segments * rank > LANES or adapters % LANES:
        return False
    if shards % COLUMNS or shards < 2 * COLUMNS or col_count > hidden:
        return False
    if not width or table_blocks(width, shrink_weight, expand_weight) * adapters > col_count:
        return False
    return 2 * hidden * col_count * 2 * shards < VMEM_BYTES - 7 * 2**20


def run_window(
    units, unit_ids, unit_live, gain_full, up_weight, down_weight, shrink_weight, expand_weight
):
    section_index = lax.axis_index("pipe")
    sections = lax.axis_size("pipe")
    unit_count = units.shape[0]
    tick_total = unit_count + sections - 1

    def process(tick_index, received, collected):
        position = jnp.clip(tick_index - section_index, 0, unit_count - 1)
        arriving = lax.dynamic_index_in_dim(
            units, jnp.minimum(tick_index, unit_count - 1), 0, keepdims=False
        )
        current = jnp.where(section_index == 0, arriving, received)
        ids_here = lax.dynamic_index_in_dim(unit_ids, position, 0, keepdims=False)
        live_here = lax.dynamic_index_in_dim(unit_live, position, 0, keepdims=False)
        produced = block_step(
            current,
            ids_here,
            live_here,
            gain_full,
            up_weight,
            down_weight,
            shrink_weight,
            expand_weight,
        )
        lag = tick_index - section_index
        in_window = jnp.logical_and(lag >= 0, lag < unit_count)
        placed = lax.dynamic_update_index_in_dim(collected, produced, position, 0)
        return (produced, jnp.where(in_window, placed, collected))

    def one_tick(tick_index, state):
        produced, collected = process(tick_index, state[0], state[1])
        return (shifted(produced, "pipe", 1), collected)

    start_state = (jnp.zeros_like(units[0]), jnp.zeros_like(units))
    received, collected = lax.fori_loop(0, tick_total - 1, one_tick, start_state)
    produced, collected = process(tick_total - 1, received, collected)
    return collected


def per_device(
    hidden_entering,
    segment_adapter,
    segment_requests,
    section_norm_gain,
    up_matrix,
    down_matrix,
    adapter_reduce,
    adapter_expand,
):
    batch_list = hidden_entering.shape[0]
    row_count = hidden_entering.shape[1]
    col_count = hidden_entering.shape[2]
    hidden = up_matrix.shape[1]
    segments = segment_adapter.shape[1]
    if batch_list == 1 and kernel_fits(
        row_count, col_count, hidden, segments, adapter_reduce[0], adapter_expand[0]
    ):
        produced = fused_sections(
            hidden_entering[0],
            segment_adapter[0],
            segment_requests[0],
            section_norm_gain[0],
            up_matrix[0],
            down_matrix[0],
            adapter_reduce[0],
            adapter_expand[0],
        )
        return produced.reshape(1, batch_list, row_count, col_count)
    collected = run_window(
        hidden_entering,
        segment_adapter,
        segment_requests,
        section_norm_gain[0],
        up_matrix[0],
        down_matrix[0],
        adapter_reduce[0],
        adapter_expand[0],
    )
    return collected.reshape(1, batch_list, row_count, col_count)


def solution(mesh):
    return jax.shard_map(
        per_device,
        mesh=mesh,
        in_specs=(
            P("rep", None, "tp"),
            P("rep", None),
            P("rep", None),
            P("pipe", None),
            P("pipe", "tp", None),
            P("pipe", "tp", None),
            P("pipe", None, "tp"),
            P("pipe", None, "tp"),
        ),
        out_specs=P("pipe", "rep", None, "tp"),
        check_vma=False,
    )
```

```python
import functools

import jax
import jax.numpy as jnp
from jax import lax
from jax.experimental import pallas as pl
from jax.experimental.pallas import tpu as pltpu
from jax.sharding import PartitionSpec as P

EPSILON = 1e-05


def shifted(x, axis, by):
    size = lax.axis_size(axis)
    pairs = [(i, i + by) for i in range(size) if 0 <= i + by < size]
    return lax.ppermute(x, axis, pairs)


def times_rows(left, weight):
    return lax.dot_general(
        left, weight, (((1,), (1,)), ((), ())), preferred_element_type=jnp.float32
    )


def block_step(
    current, unit_ids, unit_live, gain_full, up_weight, down_weight, shrink_weight, expand_weight
):
    row_count = current.shape[0]
    col_count = current.shape[1]
    hid_count = up_weight.shape[0]
    segments = unit_ids.shape[0]
    seg_rows = row_count // segments
    feature_width = gain_full.shape[0]
    adapter_rank_count = shrink_weight.shape[1] // col_count
    column = lax.axis_index("tp") * col_count
    gain_mine = lax.dynamic_slice_in_dim(gain_full, column, col_count, 0)
    widened_local = current.astype(jnp.float32)
    local_scaled = (widened_local * gain_mine).astype(jnp.bfloat16)
    input_panel = shrink_weight[unit_ids].reshape(segments, col_count, adapter_rank_count)
    output_panel = expand_weight[unit_ids].reshape(segments, hid_count, adapter_rank_count)
    partial_value = jnp.einsum(
        "sdr,spd->rsp",
        input_panel,
        local_scaled.reshape(segments, seg_rows, col_count),
        preferred_element_type=jnp.float32,
    ).reshape(adapter_rank_count, row_count)
    local_squares = jnp.sum(widened_local * widened_local, axis=1)
    reduced, squares = lax.psum((partial_value, local_squares), "tp")
    widened = lax.all_gather(current, "tp", axis=1, tiled=True).astype(jnp.float32)
    scaled = (widened * gain_full).astype(jnp.bfloat16)
    up_total = times_rows(scaled, up_weight)
    inverse = lax.rsqrt(squares / feature_width + EPSILON)
    low_rank = (
        (reduced * inverse[None, :])
        .astype(jnp.bfloat16)
        .reshape(adapter_rank_count, segments, seg_rows)
    )
    adapted = jnp.einsum(
        "rsp,sdr->spd", low_rank, output_panel, preferred_element_type=jnp.float32
    ).reshape(row_count, hid_count)
    up_sum = inverse[:, None] * up_total + adapted
    hidden_act = jax.nn.silu(up_sum).astype(jnp.bfloat16)
    down_sum = times_rows(lax.all_gather(hidden_act, "tp", axis=1, tiled=True), down_weight)
    updated = (widened_local + down_sum).astype(jnp.bfloat16)
    positions = lax.broadcasted_iota(jnp.int32, (segments, seg_rows), 1)
    row_kept = (positions < unit_live[:, None]).reshape(row_count, 1)
    return jnp.where(row_kept, updated, jnp.zeros_like(updated))


MESH = pl.DeviceIdType.MESH
PIECE = 256
COLUMNS = 2
LANES = 128
VMEM_BYTES = 67_043_328
NT = (((1,), (1,)), ((), ()))


class Spread:
    OWN, ALONG, EXTRA, ACROSS = range(4)

    def __init__(self, buf, send, recv, pieces, z, x, depth, starts_own):
        self.buf, self.send, self.recv, self.pieces = buf, send, recv, pieces
        self.z, self.x, self.depth, self.starts_own = z, x, depth, starts_own
        self.shards = depth * COLUMNS
        self.me = z * COLUMNS + x

    def copy(self, t, c, kind, target):
        return pltpu.make_async_remote_copy(
            src_ref=self.buf.at[t, c], dst_ref=self.buf.at[t, c],
            send_sem=self.send.at[kind], recv_sem=self.recv.at[t, c],
            device_id={"tp": target}, device_id_type=MESH)

    def start_along(self, source_z, t, c, kind):
        z, me = self.z, self.me

        @pl.when(jnp.logical_and(source_z <= z, z < self.depth - 1))
        def _():
            self.copy(t, c, kind, (me + COLUMNS) % self.shards).start()

        @pl.when(jnp.logical_and(source_z >= z, z > 0))
        def _():
            self.copy(t, c, kind, (me + self.shards - COLUMNS) % self.shards).start()

    def start_across(self, t, c, kind):
        self.copy(t, c, kind, self.z * COLUMNS + (1 - self.x)).start()

    def start_own(self, c):
        self.start_along(self.z, self.me, c, self.OWN)
        self.start_across(self.me, c, self.OWN)

    def arrive(self, t, c):
        self.copy(t, c, self.ACROSS, self.z * COLUMNS + (1 - self.x)).wait_recv()

    def both_sides(self, step, do):
        for source_z in (self.z - step, self.z + step) if step else (self.z,):
            @pl.when(jnp.logical_and(source_z >= 0, source_z < self.depth))
            def _():
                do(source_z)

    def relay(self, step, c):
        def do(source_z):
            t = source_z * COLUMNS + self.x
            self.arrive(t, c)
            self.start_along(source_z, t, c, self.ALONG)

            @pl.when(c < self.pieces - 1)
            def _():
                self.start_across(t, c, self.ACROSS)

        self.both_sides(step, do)

    def relay_extra(self, step):
        def do(source_z):
            t = source_z * COLUMNS + 1 - self.x
            self.arrive(t, self.pieces - 1)
            self.start_along(source_z, t, self.pieces - 1, self.EXTRA)

        self.both_sides(step, do)

    def sent(self, kind, outer, inner, filler):
        if outer and inner:
            view = filler.at[0:outer, 0:inner]
            pltpu.make_async_remote_copy(
                src_ref=view, dst_ref=view, send_sem=self.send.at[kind], recv_sem=self.recv.at[0, 0],
                device_id={"tp": self.me}, device_id_type=MESH).wait_send()

    def drain(self, filler):
        for z in range(self.depth):
            ways = (z < self.depth - 1) + (z > 0)
            layers = (z + 1) * (z < self.depth - 1) + (self.depth - z) * (z > 0)

            @pl.when(self.z == z)
            def _():
                @pl.when(self.starts_own)
                def _():
                    self.sent(self.OWN, ways + 1, self.pieces, filler)

                self.sent(self.ALONG, layers - ways, self.pieces, filler)
                self.sent(self.EXTRA, layers, 1, filler)

        self.sent(self.ACROSS, self.depth - 1, self.pieces - 1, filler)


def section_kernel(
    ids_ref, live_ref, gain_ref, x_hbm, reduce_hbm, expand_hbm, up_hbm, down_hbm, out_hbm,
    up_v, down_v, xs, act, acc, sq, shrink, expand, partial, out_v,
    up_sem, down_sem, tab_sem, own_sem, part_send, part_recv, x_send, x_recv, a_send, a_recv, h_send, out_sem,
):
    shards, x_pieces, rows, _ = xs.shape
    a_pieces = act.shape[1]
    cols = x_pieces * PIECE
    hidden = up_v.shape[0]
    width = shards * cols
    adapters, shrink_len = reduce_hbm.shape
    expand_len = expand_hbm.shape[1]
    segments = ids_ref.shape[0]
    rank = shrink_len // cols
    table_width = shards * hidden // (PIECE * rank) * (PIECE * rank)
    seg_rows = rows // segments
    depth = shards // COLUMNS
    me = lax.axis_index("tp")
    stage = lax.axis_index("pipe")
    stages = lax.axis_size("pipe")
    z, x = me // COLUMNS, me % COLUMNS
    partner = z * COLUMNS + (1 - x)
    upper = (me + COLUMNS) % shards
    lower = (me + shards - COLUMNS) % shards
    f32, bf16 = jnp.float32, jnp.bfloat16

    few = jnp.minimum(z, depth - 1 - z)
    layer = [z]
    for i in range(1, depth):
        both = i <= 2 * few
        far = jnp.where(both, (i + 1) // 2, i - few)
        down_side = jnp.where(both, i % 2 == 1, z > depth - 1 - z)
        layer.append(jnp.where(down_side, z - far, z + far))

    def shard(i, other):
        return layer[i] * COLUMNS + ((1 - x) if other else x)

    visits = [shard(i, other) for i in range(depth) for other in (False, True)]

    def up_copy(t):
        span = pl.ds(pl.multiple_of(t * cols, LANES), cols)
        return pltpu.make_async_copy(up_hbm.at[:, span], up_v.at[:, span], up_sem.at[t])

    def down_copy(t):
        span = pl.ds(pl.multiple_of(t * hidden, LANES), hidden)
        return pltpu.make_async_copy(down_hbm.at[:, span], down_v.at[:, span], down_sem.at[t])

    def own_copy(c):
        return pltpu.make_async_copy(x_hbm.at[:, c * PIECE:(c + 1) * PIECE], xs.at[me, c], own_sem.at[0])

    inner = jnp.logical_and(z > 0, z < depth - 1)
    near_other, second_other, last = shard(1, True), shard(2, True), shard(3, True)
    second_turn = jnp.where(inner, shard(3, False), near_other)
    third_turn = jnp.where(inner, near_other, shard(3, False))
    down_early = [me, partner, shard(1, False), second_turn, shard(2, False)]
    down_late = [third_turn, second_other, last]
    flat = PIECE * rank
    lane_tiles = flat // LANES

    shrink_blocks = []
    for k, at in enumerate(range(0, shrink_len, table_width)):
        size = min(table_width, shrink_len - at)
        copy = pltpu.make_async_copy(
            reduce_hbm.at[:, at:at + size],
            down_v.at[k * adapters:(k + 1) * adapters, 0:size], tab_sem.at[k])
        shrink_blocks.append((k, size, copy))
    bands = range(len(shrink_blocks), cols // adapters)
    spots = [(t, band) for t in down_late for band in bands]
    whole, rest = flat // hidden, flat % hidden
    per_spot = hidden // rest if rest else 1

    def expand_parts(n):
        parts = [(j * hidden, hidden, spots[n * whole + j], 0) for j in range(whole)]
        if rest:
            spot_of = spots[a_pieces * whole + n // per_spot]
            parts.append((whole * hidden, rest, spot_of, n % per_spot * rest))
        views = []
        for at, size, (t, band), shift in parts:
            lanes = pl.ds(pl.multiple_of(t * hidden + shift, LANES), size)
            views.append((n * flat + at, size, (slice(band * adapters, (band + 1) * adapters), lanes)))
        return views

    def start_expand():
        for n in range(a_pieces):
            for at, size, (band, lanes) in expand_parts(n):
                pltpu.make_async_copy(
                    expand_hbm.at[:, at:at + size], down_v.at[band, lanes],
                    tab_sem.at[len(shrink_blocks) + n]).start()

    def start_tables(blocks):
        for _k, _size, copy in blocks:
            copy.start()

    def start_each(copy, order):
        for t in order:
            copy(t).start()

    @pl.when(stage == 0)
    def _():
        for c in range(x_pieces):
            own_copy(c).start()
        up_copy(me).start()

    @pl.when(stage > 0)
    def _():
        start_tables(shrink_blocks)
        start_expand()
        start_each(up_copy, visits)

    barrier = pltpu.get_barrier_semaphore()

    @pl.loop(1, shards)
    def _(i):
        pl.semaphore_signal(barrier, inc=1, device_id={"tp": (me + i) % shards}, device_id_type=MESH)

    def greet(target):
        pl.semaphore_signal(
            barrier, inc=1, device_id={"pipe": stage - 1, "tp": target}, device_id_type=MESH)

    @pl.when(stage > 0)
    def _():
        greet(me)
        greet(partner)

        @pl.when(z < depth - 1)
        def _():
            greet(upper)

        @pl.when(z > 0)
        def _():
            greet(lower)

    x_side = Spread(xs, x_send, x_recv, x_pieces, z, x, depth, stage == 0)
    a_side = Spread(act, a_send, a_recv, a_pieces, z, x, depth, stage >= 0)

    def hand_over(c, target):
        return pltpu.make_async_remote_copy(
            src_ref=out_v.at[c], dst_ref=xs.at[me, c], send_sem=h_send.at[0], recv_sem=x_recv.at[me, c],
            device_id={"pipe": (stage + 1) % stages, "tp": target}, device_id_type=MESH)

    def hand_each(c):
        @pl.when(stage < stages - 1)
        def _():
            @pl.when(z < depth - 1)
            def _():
                hand_over(c, upper).start()

            @pl.when(z > 0)
            def _():
                hand_over(c, lower).start()

            hand_over(c, partner).start()
            hand_over(c, me).start()

    def hand_drain():
        for at in range(depth):
            count = 2 + (at < depth - 1) + (at > 0)

            @pl.when(jnp.logical_and(stage < stages - 1, z == at))
            def _():
                view = xs.at[0:count]
                pltpu.make_async_remote_copy(
                    src_ref=view, dst_ref=view, send_sem=h_send.at[0], recv_sem=x_recv.at[0, 0],
                    device_id={"tp": me}, device_id_type=MESH).wait_send()

    def out_copy(c):
        return pltpu.make_async_copy(out_v.at[c], out_hbm.at[:, c * PIECE:(c + 1) * PIECE], out_sem.at[0])

    row_seg = lax.broadcasted_iota(jnp.int32, (rows, LANES), 0) // seg_rows
    lane_group = lax.broadcasted_iota(jnp.int32, (rows, LANES), 1) // rank
    in_segment = row_seg == lane_group

    picks = jnp.zeros((8 * segments, adapters), f32)
    pick_row = lax.broadcasted_iota(jnp.int32, picks.shape, 0)
    pick_col = lax.broadcasted_iota(jnp.int32, picks.shape, 1)
    for s in range(segments):
        hit = jnp.logical_and(pick_row // 8 == s, pick_col == ids_ref[s])
        picks = jnp.where(hit, 1.0, picks)
    picks = picks.astype(bf16)
    spot_row = lax.broadcasted_iota(jnp.int32, (PIECE, LANES), 0) % 8
    spot_lane = lax.broadcasted_iota(jnp.int32, (PIECE, LANES), 1) // rank
    spot = spot_row == spot_lane
    fold_row = lax.broadcasted_iota(jnp.int32, (segments * LANES, LANES), 0)
    fold_col = lax.broadcasted_iota(jnp.int32, (segments * LANES, LANES), 1)
    fold = jnp.where(fold_col == fold_row // LANES * rank + fold_row % rank, 1.0, 0.0).astype(bf16)

    def panel_of(table):
        got = jnp.dot(picks, table, preferred_element_type=f32)
        parts = []
        for s in range(segments):
            tall = jnp.concatenate(
                [got[8 * s:8 * s + 8, LANES * i:LANES * (i + 1)] for i in range(lane_tiles)], axis=0)
            parts.append(jnp.where(spot, tall, 0.0).astype(bf16))
        return jnp.dot(jnp.concatenate(parts, axis=1), fold, preferred_element_type=f32).astype(bf16)

    def shrink_panels(then):
        for k, size, copy in shrink_blocks:
            copy.wait()
        start_each(up_copy, then)
        done = 0
        for k, size, copy in shrink_blocks:
            first = done

            @pl.loop(0, size // flat)
            def _(j):
                span = pl.ds(pl.multiple_of(j * flat, LANES), flat)
                at = pl.multiple_of((first + j) * PIECE, PIECE)
                shrink[pl.ds(at, PIECE), :] = panel_of(down_v[k * adapters:(k + 1) * adapters, span])

            done += size // flat

    def expand_panel(n):
        landed = down_v.at[0:adapters, 0:flat]
        pltpu.make_async_copy(landed, landed, tab_sem.at[len(shrink_blocks) + n]).wait()
        table = jnp.concatenate([down_v[band, lanes] for _at, _size, (band, lanes) in expand_parts(n)], axis=1)
        expand[n * PIECE:(n + 1) * PIECE, :] = panel_of(table)

    def raw(t, c):
        return xs[t, c].astype(f32)

    def scaled(t, c, wide):
        at = pl.multiple_of(t * cols + c * PIECE, LANES)
        return (wide * gain_ref[:, pl.ds(at, PIECE)]).astype(bf16)

    def squares(wide):
        square = wide * wide
        return square[:, :LANES] + square[:, LANES:]

    def up_tile(n, t, c):
        at = pl.multiple_of(t * cols + c * PIECE, LANES)
        return up_v[n * PIECE:(n + 1) * PIECE, pl.ds(at, PIECE)]

    def up_dot(left, n, t, c, flipped):
        dims = (((1,), (0,)), ((), ())) if flipped else NT
        return lax.dot_general(left, up_tile(n, t, c), dims, preferred_element_type=f32)

    def up_add(items, init, flipped):
        lefts = []
        total = jnp.zeros((rows, LANES), f32) if init else sq[...]
        for t, c in items:
            wide = raw(t, c)
            total += squares(wide)
            lefts.append(scaled(t, c, wide))
        sq[...] = total
        for n in range(a_pieces):
            block = slice(n * PIECE, (n + 1) * PIECE)
            part = jnp.zeros((rows, PIECE), f32)
            for (t, c), left in zip(items, lefts):
                part += up_dot(left, n, t, c, flipped)
            acc[:, block] = part if init else acc[:, block] + part

    def per_stage(work):
        @pl.when(stage == 0)
        def _():
            work(False)

        @pl.when(stage > 0)
        def _():
            work(True)

    def own_up(flipped):
        up_add([(me, c) for c in range(x_pieces)], True, flipped)

    def flip_up():
        for t in visits:
            up_copy(t).wait()

        @pl.loop(0, a_pieces * shards * x_pieces)
        def _(i):
            tall = pl.ds(pl.multiple_of(i // (shards * x_pieces) * PIECE, PIECE), PIECE)
            wide = pl.ds(pl.multiple_of(i % (shards * x_pieces) * PIECE, PIECE), PIECE)
            up_v[tall, wide] = jnp.transpose(up_v[tall, wide])

    def part_copy(owner, target):
        return pltpu.make_async_remote_copy(
            src_ref=partial.at[owner], dst_ref=partial.at[owner], send_sem=part_send.at[0],
            recv_sem=part_recv.at[0], device_id={"tp": target}, device_id_type=MESH)

    def send_part():
        low = jnp.zeros((rows, LANES), f32)
        for c in range(x_pieces):
            low += jnp.dot(scaled(me, c, raw(me, c)), shrink[c * PIECE:(c + 1) * PIECE, :],
                           preferred_element_type=f32)
        low = jnp.where(in_segment, low, 0.0)
        if rows < LANES:
            low = jnp.concatenate([low, jnp.zeros((LANES - rows, LANES), f32)], axis=0)
        turned = jnp.transpose(low)
        picked = turned[0:rank]
        for s in range(1, segments):
            picked = picked + turned[s * rank:(s + 1) * rank]
        partial[me] = picked

        @pl.loop(1, shards)
        def _(i):
            part_copy(me, (me + i) % shards).start()

    @pl.when(stage == 0)
    def _():
        pltpu.make_async_copy(xs.at[me], xs.at[me], own_sem.at[0]).wait()
        up_copy(me).wait()
        start_tables(shrink_blocks)
        own_up(False)
        start_each(up_copy, visits[1:3])

    fed = 2 + jnp.where(z < depth - 1, 1, 0) + jnp.where(z > 0, 1, 0)
    pl.semaphore_wait(barrier, shards - 1 + jnp.where(stage < stages - 1, fed, 0))

    @pl.when(stage == 0)
    def _():
        for c in range(x_pieces):
            x_side.start_own(c)
        shrink_panels(visits[3:5])
        send_part()

    @pl.when(stage > 0)
    def _():
        shrink_panels([])
        for n in range(a_pieces):
            expand_panel(n)
        start_each(down_copy, down_early + down_late)
        flip_up()

    @pl.when(stage > 0)
    def _():
        for c in range(x_pieces):
            x_side.arrive(me, c)
        own_up(True)

    def first_relay(side, c):
        side.relay(1, c)

        @pl.when(c < side.pieces - 1)
        def _():
            side.arrive(partner, c)

        @pl.when(c == side.pieces - 1)
        def _():
            side.relay_extra(0)

    def second_relay(side, c):
        side.relay(2, c)

        @pl.when(jnp.logical_and(c < side.pieces - 1, jnp.logical_not(inner)))
        def _():
            side.arrive(near_other, c)

        @pl.when(c == side.pieces - 1)
        def _():
            side.relay_extra(1)

    def third_relay(side, c, full):
        side.relay(3, c)
        if full:
            @pl.when(inner)
            def _():
                side.arrive(near_other, c)

            side.arrive(second_other, c)
        else:
            @pl.when(inner)
            def _():
                side.relay_extra(2)

    def end_extras(side):
        @pl.when(jnp.logical_not(inner))
        def _():
            side.relay_extra(2)

        side.relay_extra(3)

    def up_more(*items):
        per_stage(functools.partial(up_add, list(items), False))

    @pl.when(stage == 0)
    def _():
        for t in (partner, shard(1, False)):
            up_copy(t).wait()
        start_each(up_copy, visits[5:])

    pair = 2
    end = x_pieces - 1

    @pl.loop(0, x_pieces // pair)
    def _(j):
        for c in (pair * j, pair * j + 1):
            first_relay(x_side, c)
        up_more(*[(t, pair * j + g) for t in (partner, shard(1, False)) for g in range(pair)])

    @pl.when(stage > 0)
    def _():
        send_part()

    @pl.when(stage == 0)
    def _():
        start_expand()
        for t in visits[3:5]:
            up_copy(t).wait()

        @pl.when(inner)
        def _():
            up_copy(shard(3, False)).wait()

    @pl.loop(0, x_pieces // pair)
    def _(j):
        for c in (pair * j, pair * j + 1):
            second_relay(x_side, c)
        up_more(*[(t, pair * j + g) for t in (second_turn, shard(2, False)) for g in range(pair)])

    @pl.when(stage == 0)
    def _():
        start_each(down_copy, down_early)
        up_copy(second_other).wait()

        @pl.when(jnp.logical_not(inner))
        def _():
            up_copy(shard(3, False)).wait()

    for c in range(0, x_pieces - pair, pair):
        for g in range(pair):
            third_relay(x_side, c + g, True)
        up_more(*[(t, c + g) for t in (third_turn, second_other) for g in range(pair)])
    third_relay(x_side, end - 1, True)
    third_relay(x_side, end, False)

    @pl.when(stage == 0)
    def _():
        up_copy(last).wait()

    for c in range(end - 2):
        x_side.arrive(last, c)
    up_more((third_turn, end - 1), (third_turn, end), (second_other, end - 1), *[(last, c) for c in range(end - 2)])

    x_side.arrive(last, end - 2)
    end_extras(x_side)
    up_more((last, end - 2), (second_other, end), (last, end))

    others = partial.at[0:shards - 1]
    all_parts = pltpu.make_async_remote_copy(
        src_ref=others, dst_ref=others, send_sem=part_send.at[0], recv_sem=part_recv.at[0],
        device_id={"tp": me}, device_id_type=MESH)
    all_parts.wait_recv()

    summed = partial[0]
    for t in range(1, shards):
        summed = summed + partial[t]
    stacked = jnp.concatenate([summed] * segments + [jnp.zeros((LANES - segments * rank, LANES), f32)], axis=0)
    low = jnp.where(in_segment, jnp.transpose(stacked)[:rows], 0.0)

    @pl.when(stage == 0)
    def _():
        expand_panel(0)

    x_side.arrive(last, end - 1)
    finals = [(last, end - 1)]
    square = sq[...]
    lefts = []
    for t, c in finals:
        wide = raw(t, c)
        square += squares(wide)
        lefts.append(scaled(t, c, wide))
    inverse = lax.rsqrt(jnp.sum(square, axis=1, keepdims=True) / width + EPSILON)
    low_rank = (low * inverse).astype(bf16)

    lag = 4

    def up_finish(flipped):
        for n in range(a_pieces):
            block = slice(n * PIECE, (n + 1) * PIECE)
            base = jnp.zeros((rows, PIECE), f32)
            for (t, c), left in zip(finals, lefts):
                base += up_dot(left, n, t, c, flipped)
            if n and not flipped:
                expand_panel(n)
            adapted = lax.dot_general(low_rank, expand[block, :], NT, preferred_element_type=f32)
            value = inverse * (acc[:, block] + base) + adapted
            act[me, n] = (value / (1.0 + jnp.exp(-value))).astype(bf16)
            a_side.start_own(n)
            if n >= lag and not flipped:
                first_relay(a_side, jnp.int32(n - lag))

    per_stage(up_finish)

    def down_tile(n, t, c):
        at = pl.multiple_of(t * hidden + c * PIECE, LANES)
        return down_v[n * PIECE:(n + 1) * PIECE, pl.ds(at, PIECE)]

    def down_add(items):
        for n in range(x_pieces):
            block = slice(n * PIECE, (n + 1) * PIECE)
            part = jnp.zeros((rows, PIECE), f32)
            for t, c in items:
                part += lax.dot_general(act[t, c], down_tile(n, t, c), NT, preferred_element_type=f32)
            acc[:, block] = acc[:, block] + part

    @pl.when(stage == 0)
    def _():
        start_each(down_copy, down_late)

    for n in range(x_pieces):
        acc[:, n * PIECE:(n + 1) * PIECE] = xs[me, n].astype(f32)

    for t in down_early[:3]:
        down_copy(t).wait()
    end = a_pieces - 1

    @pl.loop(0, a_pieces)
    def _(c):
        @pl.when(jnp.logical_or(stage > 0, c >= a_pieces - lag))
        def _():
            first_relay(a_side, c)

        down_add([(me, c), (partner, c), (shard(1, False), c)])

    for t in down_early[3:]:
        down_copy(t).wait()

    @pl.loop(0, a_pieces)
    def _(c):
        second_relay(a_side, c)
        down_add([(second_turn, c), (shard(2, False), c)])

    for t in down_late:
        down_copy(t).wait()

    late = max(end - 2, 0)

    @pl.loop(0, late)
    def _(c):
        third_relay(a_side, c, True)
        down_add([(third_turn, c), (second_other, c)])

    @pl.loop(late, end)
    def _(c):
        third_relay(a_side, c, True)
        a_side.arrive(last, c - late)
        down_add([(third_turn, c), (second_other, c), (last, c - late)])

    third_relay(a_side, end, False)
    a_side.arrive(last, end - late)
    down_add([(third_turn, end), (last, end - late)])
    rest = list(range(end - late + 1, end - 1))
    for c in rest:
        a_side.arrive(last, c)
    down_add([(last, c) for c in rest])
    end_extras(a_side)
    down_add([(second_other, end), (last, end)])

    row = lax.broadcasted_iota(jnp.int32, (rows, 1), 0)
    kept = row < 0
    for s in range(segments):
        start = s * seg_rows
        kept = jnp.logical_or(kept, jnp.logical_and(row >= start, row < start + jnp.minimum(live_ref[s], seg_rows)))

    a_side.arrive(last, end - 1)
    for n in range(x_pieces):
        block = slice(n * PIECE, (n + 1) * PIECE)
        part = jnp.zeros((rows, PIECE), f32)
        part += lax.dot_general(act[last, end - 1], down_tile(n, last, end - 1), NT, preferred_element_type=f32)
        out_v[n] = jnp.where(kept, acc[:, block] + part, 0.0).astype(bf16)
        hand_each(n)
        out_copy(n).start()

    all_parts.wait_send()
    x_side.drain(act)
    a_side.drain(act)
    hand_drain()
    pltpu.make_async_copy(out_v, out_v, out_sem.at[0]).wait()


def fused_sections(current, ids, live, gain, up_weight, down_weight, shrink_weight, expand_weight):
    rows, cols = current.shape
    hidden = up_weight.shape[0]
    shards = lax.axis_size("tp")
    rank = shrink_weight.shape[1] // cols
    x_pieces, a_pieces = cols // PIECE, hidden // PIECE
    vmem = pl.BlockSpec(memory_space=pltpu.VMEM)
    smem = pl.BlockSpec(memory_space=pltpu.SMEM)
    hbm = pl.BlockSpec(memory_space=pl.ANY)
    dma = pltpu.SemaphoreType.DMA
    flat = PIECE * rank
    blocks = table_blocks(shards * hidden // flat * flat, shrink_weight) + a_pieces
    return pl.pallas_call(
        section_kernel,
        out_shape=jax.ShapeDtypeStruct((rows, cols), jnp.bfloat16),
        in_specs=[smem, smem, vmem] + [hbm] * 5,
        out_specs=hbm,
        scratch_shapes=[
            pltpu.VMEM(up_weight.shape, jnp.bfloat16),
            pltpu.VMEM(down_weight.shape, jnp.bfloat16),
            pltpu.VMEM((shards, x_pieces, rows, PIECE), jnp.bfloat16),
            pltpu.VMEM((shards, a_pieces, rows, PIECE), jnp.bfloat16),
            pltpu.VMEM((rows, hidden), jnp.float32),
            pltpu.VMEM((rows, LANES), jnp.float32),
            pltpu.VMEM((cols, LANES), jnp.bfloat16),
            pltpu.VMEM((hidden, LANES), jnp.bfloat16),
            pltpu.VMEM((shards, rank, LANES), jnp.float32),
            pltpu.VMEM((x_pieces, rows, PIECE), jnp.bfloat16),
            dma((shards,)), dma((shards,)), dma((blocks,)), dma((1,)),
            dma((1,)), dma((1,)),
            dma((4,)), dma((shards, x_pieces)),
            dma((4,)), dma((shards, a_pieces)),
            dma((1,)), dma((1,)),
        ],
        compiler_params=pltpu.CompilerParams(
            collective_id=0, has_side_effects=True, vmem_limit_bytes=VMEM_BYTES
        ),
    )(ids, live, gain[None, :], current, shrink_weight, expand_weight, up_weight, down_weight)


def table_blocks(width, *tables):
    return sum(-(-table.shape[1] // width) for table in tables)


def kernel_fits(row_count, col_count, hidden, segments, shrink_weight, expand_weight):
    shards = lax.axis_size("tp")
    adapters, flat_cols = shrink_weight.shape
    rank = flat_cols // col_count
    flat = PIECE * rank
    width = shards * hidden // flat * flat
    if col_count % PIECE or hidden % PIECE or hidden < 5 * PIECE or col_count // PIECE != 4:
        return False
    if row_count > LANES or rank * 8 != LANES or segments * rank > LANES or adapters % LANES:
        return False
    if shards != 4 * COLUMNS or col_count > hidden:
        return False
    if not width or hidden % LANES:
        return False
    whole, rest = flat // hidden, flat % hidden
    spots = 3 * (col_count // adapters - table_blocks(width, shrink_weight))
    pieces = hidden // PIECE
    if pieces * whole + (-(-pieces // (hidden // rest)) if rest else 0) > spots:
        return False
    return 2 * hidden * col_count * 2 * shards < VMEM_BYTES - 7 * 2**20


def run_window(
    units, unit_ids, unit_live, gain_full, up_weight, down_weight, shrink_weight, expand_weight
):
    section_index = lax.axis_index("pipe")
    sections = lax.axis_size("pipe")
    unit_count = units.shape[0]
    tick_total = unit_count + sections - 1

    def process(tick_index, received, collected):
        position = jnp.clip(tick_index - section_index, 0, unit_count - 1)
        arriving = lax.dynamic_index_in_dim(
            units, jnp.minimum(tick_index, unit_count - 1), 0, keepdims=False
        )
        current = jnp.where(section_index == 0, arriving, received)
        ids_here = lax.dynamic_index_in_dim(unit_ids, position, 0, keepdims=False)
        live_here = lax.dynamic_index_in_dim(unit_live, position, 0, keepdims=False)
        produced = block_step(
            current,
            ids_here,
            live_here,
            gain_full,
            up_weight,
            down_weight,
            shrink_weight,
            expand_weight,
        )
        lag = tick_index - section_index
        in_window = jnp.logical_and(lag >= 0, lag < unit_count)
        placed = lax.dynamic_update_index_in_dim(collected, produced, position, 0)
        return (produced, jnp.where(in_window, placed, collected))

    def one_tick(tick_index, state):
        produced, collected = process(tick_index, state[0], state[1])
        return (shifted(produced, "pipe", 1), collected)

    start_state = (jnp.zeros_like(units[0]), jnp.zeros_like(units))
    received, collected = lax.fori_loop(0, tick_total - 1, one_tick, start_state)
    produced, collected = process(tick_total - 1, received, collected)
    return collected


def per_device(
    hidden_entering,
    segment_adapter,
    segment_requests,
    section_norm_gain,
    up_matrix,
    down_matrix,
    adapter_reduce,
    adapter_expand,
):
    batch_list = hidden_entering.shape[0]
    row_count = hidden_entering.shape[1]
    col_count = hidden_entering.shape[2]
    hidden = up_matrix.shape[1]
    segments = segment_adapter.shape[1]
    if batch_list == 1 and kernel_fits(
        row_count, col_count, hidden, segments, adapter_reduce[0], adapter_expand[0]
    ):
        produced = fused_sections(
            hidden_entering[0],
            segment_adapter[0],
            segment_requests[0],
            section_norm_gain[0],
            up_matrix[0],
            down_matrix[0],
            adapter_reduce[0],
            adapter_expand[0],
        )
        return produced.reshape(1, batch_list, row_count, col_count)
    collected = run_window(
        hidden_entering,
        segment_adapter,
        segment_requests,
        section_norm_gain[0],
        up_matrix[0],
        down_matrix[0],
        adapter_reduce[0],
        adapter_expand[0],
    )
    return collected.reshape(1, batch_list, row_count, col_count)


def solution(mesh):
    return jax.shard_map(
        per_device,
        mesh=mesh,
        in_specs=(
            P("rep", None, "tp"),
            P("rep", None),
            P("rep", None),
            P("pipe", None),
            P("pipe", "tp", None),
            P("pipe", "tp", None),
            P("pipe", None, "tp"),
            P("pipe", None, "tp"),
        ),
        out_specs=P("pipe", "rep", None, "tp"),
        check_vma=False,
    )
```

```python
import functools

import jax
import jax.numpy as jnp
from jax import lax
from jax.experimental import pallas as pl
from jax.experimental.pallas import tpu as pltpu
from jax.sharding import PartitionSpec as P

EPSILON = 1e-05


def shifted(x, axis, by):
    size = lax.axis_size(axis)
    pairs = [(i, i + by) for i in range(size) if 0 <= i + by < size]
    return lax.ppermute(x, axis, pairs)


def times_rows(left, weight):
    return lax.dot_general(
        left, weight, (((1,), (1,)), ((), ())), preferred_element_type=jnp.float32
    )


def block_step(
    current, unit_ids, unit_live, gain_full, up_weight, down_weight, shrink_weight, expand_weight
):
    row_count = current.shape[0]
    col_count = current.shape[1]
    hid_count = up_weight.shape[0]
    segments = unit_ids.shape[0]
    seg_rows = row_count // segments
    feature_width = gain_full.shape[0]
    adapter_rank_count = shrink_weight.shape[1] // col_count
    column = lax.axis_index("tp") * col_count
    gain_mine = lax.dynamic_slice_in_dim(gain_full, column, col_count, 0)
    widened_local = current.astype(jnp.float32)
    local_scaled = (widened_local * gain_mine).astype(jnp.bfloat16)
    input_panel = shrink_weight[unit_ids].reshape(segments, col_count, adapter_rank_count)
    output_panel = expand_weight[unit_ids].reshape(segments, hid_count, adapter_rank_count)
    partial_value = jnp.einsum(
        "sdr,spd->rsp",
        input_panel,
        local_scaled.reshape(segments, seg_rows, col_count),
        preferred_element_type=jnp.float32,
    ).reshape(adapter_rank_count, row_count)
    local_squares = jnp.sum(widened_local * widened_local, axis=1)
    reduced, squares = lax.psum((partial_value, local_squares), "tp")
    widened = lax.all_gather(current, "tp", axis=1, tiled=True).astype(jnp.float32)
    scaled = (widened * gain_full).astype(jnp.bfloat16)
    up_total = times_rows(scaled, up_weight)
    inverse = lax.rsqrt(squares / feature_width + EPSILON)
    low_rank = (
        (reduced * inverse[None, :])
        .astype(jnp.bfloat16)
        .reshape(adapter_rank_count, segments, seg_rows)
    )
    adapted = jnp.einsum(
        "rsp,sdr->spd", low_rank, output_panel, preferred_element_type=jnp.float32
    ).reshape(row_count, hid_count)
    up_sum = inverse[:, None] * up_total + adapted
    hidden_act = jax.nn.silu(up_sum).astype(jnp.bfloat16)
    down_sum = times_rows(lax.all_gather(hidden_act, "tp", axis=1, tiled=True), down_weight)
    updated = (widened_local + down_sum).astype(jnp.bfloat16)
    positions = lax.broadcasted_iota(jnp.int32, (segments, seg_rows), 1)
    row_kept = (positions < unit_live[:, None]).reshape(row_count, 1)
    return jnp.where(row_kept, updated, jnp.zeros_like(updated))


MESH = pl.DeviceIdType.MESH
PIECE = 256
COLUMNS = 2
LANES = 128
VMEM_BYTES = 67_043_328
NT = (((1,), (1,)), ((), ()))


class Spread:
    OWN, ALONG, EXTRA, ACROSS = range(4)

    def __init__(self, buf, send, recv, pieces, z, x, depth, starts_own):
        self.buf, self.send, self.recv, self.pieces = buf, send, recv, pieces
        self.z, self.x, self.depth, self.starts_own = z, x, depth, starts_own
        self.shards = depth * COLUMNS
        self.me = z * COLUMNS + x

    def copy(self, t, c, kind, target):
        return pltpu.make_async_remote_copy(
            src_ref=self.buf.at[t, c], dst_ref=self.buf.at[t, c],
            send_sem=self.send.at[kind], recv_sem=self.recv.at[t, c],
            device_id={"tp": target}, device_id_type=MESH)

    def start_along(self, source_z, t, c, kind):
        z, me = self.z, self.me

        @pl.when(jnp.logical_and(source_z <= z, z < self.depth - 1))
        def _():
            self.copy(t, c, kind, (me + COLUMNS) % self.shards).start()

        @pl.when(jnp.logical_and(source_z >= z, z > 0))
        def _():
            self.copy(t, c, kind, (me + self.shards - COLUMNS) % self.shards).start()

    def start_across(self, t, c, kind):
        self.copy(t, c, kind, self.z * COLUMNS + (1 - self.x)).start()

    def start_own(self, c):
        self.start_along(self.z, self.me, c, self.OWN)
        self.start_across(self.me, c, self.OWN)

    def arrive(self, t, c):
        self.copy(t, c, self.ACROSS, self.z * COLUMNS + (1 - self.x)).wait_recv()

    def both_sides(self, step, do):
        for source_z in (self.z - step, self.z + step) if step else (self.z,):
            @pl.when(jnp.logical_and(source_z >= 0, source_z < self.depth))
            def _():
                do(source_z)

    def relay(self, step, c):
        def do(source_z):
            t = source_z * COLUMNS + self.x
            self.arrive(t, c)
            self.start_along(source_z, t, c, self.ALONG)

            @pl.when(c < self.pieces - 1)
            def _():
                self.start_across(t, c, self.ACROSS)

        self.both_sides(step, do)

    def relay_extra(self, step):
        def do(source_z):
            t = source_z * COLUMNS + 1 - self.x
            self.arrive(t, self.pieces - 1)
            self.start_along(source_z, t, self.pieces - 1, self.EXTRA)

        self.both_sides(step, do)

    def sent(self, kind, outer, inner, filler):
        if outer and inner:
            view = filler.at[0:outer, 0:inner]
            pltpu.make_async_remote_copy(
                src_ref=view, dst_ref=view, send_sem=self.send.at[kind], recv_sem=self.recv.at[0, 0],
                device_id={"tp": self.me}, device_id_type=MESH).wait_send()

    def drain(self, filler):
        for z in range(self.depth):
            ways = (z < self.depth - 1) + (z > 0)
            layers = (z + 1) * (z < self.depth - 1) + (self.depth - z) * (z > 0)

            @pl.when(self.z == z)
            def _():
                @pl.when(self.starts_own)
                def _():
                    self.sent(self.OWN, ways + 1, self.pieces, filler)

                self.sent(self.ALONG, layers - ways, self.pieces, filler)
                self.sent(self.EXTRA, layers, 1, filler)

        self.sent(self.ACROSS, self.depth - 1, self.pieces - 1, filler)


def section_kernel(
    ids_ref, live_ref, gain_ref, x_hbm, reduce_hbm, expand_hbm, up_hbm, down_hbm, out_hbm,
    up_v, down_v, xs, act, acc, sq, shrink, expand, partial, out_v,
    up_sem, down_sem, tab_sem, own_sem, part_send, part_recv, x_send, x_recv, a_send, a_recv, h_send, out_sem,
):
    shards, x_pieces, rows, _ = xs.shape
    a_pieces = act.shape[1]
    cols = x_pieces * PIECE
    hidden = up_v.shape[0]
    width = shards * cols
    adapters, shrink_len = reduce_hbm.shape
    expand_len = expand_hbm.shape[1]
    segments = ids_ref.shape[0]
    rank = shrink_len // cols
    table_width = shards * hidden // (PIECE * rank) * (PIECE * rank)
    seg_rows = rows // segments
    depth = shards // COLUMNS
    me = lax.axis_index("tp")
    stage = lax.axis_index("pipe")
    stages = lax.axis_size("pipe")
    z, x = me // COLUMNS, me % COLUMNS
    partner = z * COLUMNS + (1 - x)
    upper = (me + COLUMNS) % shards
    lower = (me + shards - COLUMNS) % shards
    f32, bf16 = jnp.float32, jnp.bfloat16

    few = jnp.minimum(z, depth - 1 - z)
    layer = [z]
    for i in range(1, depth):
        both = i <= 2 * few
        far = jnp.where(both, (i + 1) // 2, i - few)
        down_side = jnp.where(both, i % 2 == 1, z > depth - 1 - z)
        layer.append(jnp.where(down_side, z - far, z + far))

    def shard(i, other):
        return layer[i] * COLUMNS + ((1 - x) if other else x)

    visits = [shard(i, other) for i in range(depth) for other in (False, True)]

    def up_copy(t):
        span = pl.ds(pl.multiple_of(t * cols, LANES), cols)
        return pltpu.make_async_copy(up_hbm.at[:, span], up_v.at[:, span], up_sem.at[t])

    def down_copy(t):
        span = pl.ds(pl.multiple_of(t * hidden, LANES), hidden)
        return pltpu.make_async_copy(down_hbm.at[:, span], down_v.at[:, span], down_sem.at[t])

    def own_copy(c):
        return pltpu.make_async_copy(x_hbm.at[:, c * PIECE:(c + 1) * PIECE], xs.at[me, c], own_sem.at[0])

    inner = jnp.logical_and(z > 0, z < depth - 1)
    near_other, second_other, last = shard(1, True), shard(2, True), shard(3, True)
    second_turn = jnp.where(inner, shard(3, False), near_other)
    third_turn = jnp.where(inner, near_other, shard(3, False))
    down_early = [me, partner, shard(1, False), second_turn, shard(2, False)]
    down_late = [third_turn, second_other, last]
    flat = PIECE * rank
    lane_tiles = flat // LANES

    shrink_blocks = []
    for k, at in enumerate(range(0, shrink_len, table_width)):
        size = min(table_width, shrink_len - at)
        copy = pltpu.make_async_copy(
            reduce_hbm.at[:, at:at + size],
            down_v.at[k * adapters:(k + 1) * adapters, 0:size], tab_sem.at[k])
        shrink_blocks.append((k, size, copy))
    bands = range(len(shrink_blocks), cols // adapters)
    spots = [(t, band) for t in down_late for band in bands]
    whole, rest = flat // hidden, flat % hidden
    per_spot = hidden // rest if rest else 1

    def expand_parts(n):
        parts = [(j * hidden, hidden, spots[n * whole + j], 0) for j in range(whole)]
        if rest:
            spot_of = spots[a_pieces * whole + n // per_spot]
            parts.append((whole * hidden, rest, spot_of, n % per_spot * rest))
        views = []
        for at, size, (t, band), shift in parts:
            lanes = pl.ds(pl.multiple_of(t * hidden + shift, LANES), size)
            views.append((n * flat + at, size, (slice(band * adapters, (band + 1) * adapters), lanes)))
        return views

    def start_expand():
        for n in range(a_pieces):
            for at, size, (band, lanes) in expand_parts(n):
                pltpu.make_async_copy(
                    expand_hbm.at[:, at:at + size], down_v.at[band, lanes],
                    tab_sem.at[len(shrink_blocks) + n]).start()

    def start_tables(blocks):
        for _k, _size, copy in blocks:
            copy.start()

    def start_each(copy, order):
        for t in order:
            copy(t).start()

    @pl.when(stage == 0)
    def _():
        for c in range(x_pieces):
            own_copy(c).start()
        up_copy(me).start()

    @pl.when(stage > 0)
    def _():
        start_tables(shrink_blocks)
        start_expand()
        start_each(up_copy, visits)

    barrier = pltpu.get_barrier_semaphore()

    @pl.loop(1, shards)
    def _(i):
        pl.semaphore_signal(barrier, inc=1, device_id={"tp": (me + i) % shards}, device_id_type=MESH)

    def greet(target):
        pl.semaphore_signal(
            barrier, inc=1, device_id={"pipe": stage - 1, "tp": target}, device_id_type=MESH)

    @pl.when(stage > 0)
    def _():
        greet(me)
        greet(partner)

        @pl.when(z < depth - 1)
        def _():
            greet(upper)

        @pl.when(z > 0)
        def _():
            greet(lower)

    x_side = Spread(xs, x_send, x_recv, x_pieces, z, x, depth, stage == 0)
    a_side = Spread(act, a_send, a_recv, a_pieces, z, x, depth, stage >= 0)

    def hand_over(c, target):
        return pltpu.make_async_remote_copy(
            src_ref=out_v.at[c], dst_ref=xs.at[me, c], send_sem=h_send.at[0], recv_sem=x_recv.at[me, c],
            device_id={"pipe": (stage + 1) % stages, "tp": target}, device_id_type=MESH)

    def hand_each(c):
        @pl.when(stage < stages - 1)
        def _():
            @pl.when(z < depth - 1)
            def _():
                hand_over(c, upper).start()

            @pl.when(z > 0)
            def _():
                hand_over(c, lower).start()

            hand_over(c, partner).start()
            hand_over(c, me).start()

    def hand_drain():
        for at in range(depth):
            count = 2 + (at < depth - 1) + (at > 0)

            @pl.when(jnp.logical_and(stage < stages - 1, z == at))
            def _():
                view = xs.at[0:count]
                pltpu.make_async_remote_copy(
                    src_ref=view, dst_ref=view, send_sem=h_send.at[0], recv_sem=x_recv.at[0, 0],
                    device_id={"tp": me}, device_id_type=MESH).wait_send()

    def out_copy(c):
        return pltpu.make_async_copy(out_v.at[c], out_hbm.at[:, c * PIECE:(c + 1) * PIECE], out_sem.at[0])

    row_seg = lax.broadcasted_iota(jnp.int32, (rows, LANES), 0) // seg_rows
    lane_group = lax.broadcasted_iota(jnp.int32, (rows, LANES), 1) // rank
    in_segment = row_seg == lane_group

    picks = jnp.zeros((8 * segments, adapters), f32)
    pick_row = lax.broadcasted_iota(jnp.int32, picks.shape, 0)
    pick_col = lax.broadcasted_iota(jnp.int32, picks.shape, 1)
    for s in range(segments):
        hit = jnp.logical_and(pick_row // 8 == s, pick_col == ids_ref[s])
        picks = jnp.where(hit, 1.0, picks)
    picks = picks.astype(bf16)
    spot_row = lax.broadcasted_iota(jnp.int32, (PIECE, LANES), 0) % 8
    spot_lane = lax.broadcasted_iota(jnp.int32, (PIECE, LANES), 1) // rank
    spot = spot_row == spot_lane
    fold_row = lax.broadcasted_iota(jnp.int32, (segments * LANES, LANES), 0)
    fold_col = lax.broadcasted_iota(jnp.int32, (segments * LANES, LANES), 1)
    fold = jnp.where(fold_col == fold_row // LANES * rank + fold_row % rank, 1.0, 0.0).astype(bf16)

    def panel_of(table):
        got = jnp.dot(picks, table, preferred_element_type=f32)
        parts = []
        for s in range(segments):
            tall = jnp.concatenate(
                [got[8 * s:8 * s + 8, LANES * i:LANES * (i + 1)] for i in range(lane_tiles)], axis=0)
            parts.append(jnp.where(spot, tall, 0.0).astype(bf16))
        return jnp.dot(jnp.concatenate(parts, axis=1), fold, preferred_element_type=f32).astype(bf16)

    def shrink_panels(then):
        for k, size, copy in shrink_blocks:
            copy.wait()
        then()
        done = 0
        for k, size, copy in shrink_blocks:
            first = done

            @pl.loop(0, size // flat)
            def _(j):
                span = pl.ds(pl.multiple_of(j * flat, LANES), flat)
                at = pl.multiple_of((first + j) * PIECE, PIECE)
                shrink[pl.ds(at, PIECE), :] = panel_of(down_v[k * adapters:(k + 1) * adapters, span])

            done += size // flat

    def expand_panel(n):
        landed = down_v.at[0:adapters, 0:flat]
        pltpu.make_async_copy(landed, landed, tab_sem.at[len(shrink_blocks) + n]).wait()
        table = jnp.concatenate([down_v[band, lanes] for _at, _size, (band, lanes) in expand_parts(n)], axis=1)
        expand[n * PIECE:(n + 1) * PIECE, :] = panel_of(table)

    def raw(t, c):
        return xs[t, c].astype(f32)

    def scaled(t, c, wide):
        at = pl.multiple_of(t * cols + c * PIECE, LANES)
        return (wide * gain_ref[:, pl.ds(at, PIECE)]).astype(bf16)

    def squares(wide):
        square = wide * wide
        return square[:, :LANES] + square[:, LANES:]

    def up_tile(n, t, c):
        at = pl.multiple_of(t * cols + c * PIECE, LANES)
        return up_v[n * PIECE:(n + 1) * PIECE, pl.ds(at, PIECE)]

    def up_dot(left, n, t, c, flipped):
        dims = (((1,), (0,)), ((), ())) if flipped else NT
        return lax.dot_general(left, up_tile(n, t, c), dims, preferred_element_type=f32)

    def up_add(items, init, flipped):
        lefts = []
        total = jnp.zeros((rows, LANES), f32) if init else sq[...]
        for t, c in items:
            wide = raw(t, c)
            total += squares(wide)
            lefts.append(scaled(t, c, wide))
        sq[...] = total
        for n in range(a_pieces):
            block = slice(n * PIECE, (n + 1) * PIECE)
            part = jnp.zeros((rows, PIECE), f32)
            for (t, c), left in zip(items, lefts):
                part += up_dot(left, n, t, c, flipped)
            acc[:, block] = part if init else acc[:, block] + part

    def per_stage(work):
        @pl.when(stage == 0)
        def _():
            work(False)

        @pl.when(stage > 0)
        def _():
            work(True)

    def own_up(flipped):
        up_add([(me, c) for c in range(x_pieces)], True, flipped)

    def flip_up():
        for t in visits:
            up_copy(t).wait()

        @pl.loop(0, a_pieces * shards * x_pieces)
        def _(i):
            tall = pl.ds(pl.multiple_of(i // (shards * x_pieces) * PIECE, PIECE), PIECE)
            wide = pl.ds(pl.multiple_of(i % (shards * x_pieces) * PIECE, PIECE), PIECE)
            up_v[tall, wide] = jnp.transpose(up_v[tall, wide])

    def part_copy(owner, target):
        return pltpu.make_async_remote_copy(
            src_ref=partial.at[owner], dst_ref=partial.at[owner], send_sem=part_send.at[0],
            recv_sem=part_recv.at[0], device_id={"tp": target}, device_id_type=MESH)

    def send_part():
        low = jnp.zeros((rows, LANES), f32)
        for c in range(x_pieces):
            low += jnp.dot(scaled(me, c, raw(me, c)), shrink[c * PIECE:(c + 1) * PIECE, :],
                           preferred_element_type=f32)
        low = jnp.where(in_segment, low, 0.0)
        if rows < LANES:
            low = jnp.concatenate([low, jnp.zeros((LANES - rows, LANES), f32)], axis=0)
        turned = jnp.transpose(low)
        picked = turned[0:rank]
        for s in range(1, segments):
            picked = picked + turned[s * rank:(s + 1) * rank]
        partial[me] = picked

        @pl.loop(1, shards)
        def _(i):
            part_copy(me, (me + i) % shards).start()

    @pl.when(stage == 0)
    def _():
        pltpu.make_async_copy(xs.at[me], xs.at[me], own_sem.at[0]).wait()
        up_copy(me).wait()
        start_tables(shrink_blocks)
        own_up(False)
        start_each(up_copy, visits[1:3])

    fed = 2 + jnp.where(z < depth - 1, 1, 0) + jnp.where(z > 0, 1, 0)
    pl.semaphore_wait(barrier, shards - 1 + jnp.where(stage < stages - 1, fed, 0))

    @pl.when(stage == 0)
    def _():
        for c in range(x_pieces):
            x_side.start_own(c)
        shrink_panels(lambda: start_each(up_copy, visits[3:5] + visits[6:7]))
        send_part()

    @pl.when(stage > 0)
    def _():
        shrink_panels(lambda: None)
        for n in range(a_pieces):
            expand_panel(n)
        start_each(down_copy, down_early + down_late)
        flip_up()

    @pl.when(stage > 0)
    def _():
        for c in range(x_pieces):
            x_side.arrive(me, c)
        own_up(True)

    def first_relay(side, c):
        side.relay(1, c)

        @pl.when(c < side.pieces - 1)
        def _():
            side.arrive(partner, c)

        @pl.when(c == side.pieces - 1)
        def _():
            side.relay_extra(0)

    def second_relay(side, c):
        side.relay(2, c)

        @pl.when(jnp.logical_and(c < side.pieces - 1, jnp.logical_not(inner)))
        def _():
            side.arrive(near_other, c)

        @pl.when(c == side.pieces - 1)
        def _():
            side.relay_extra(1)

    def third_relay(side, c, full):
        side.relay(3, c)
        if full:
            @pl.when(inner)
            def _():
                side.arrive(near_other, c)

            side.arrive(second_other, c)
        else:
            @pl.when(inner)
            def _():
                side.relay_extra(2)

    def end_extras(side):
        @pl.when(jnp.logical_not(inner))
        def _():
            side.relay_extra(2)

        side.relay_extra(3)

    def up_more(*items):
        per_stage(functools.partial(up_add, list(items), False))

    @pl.when(stage == 0)
    def _():
        for t in (partner, shard(1, False)):
            up_copy(t).wait()
        start_expand()

    pair = 2
    end = x_pieces - 1

    @pl.loop(0, x_pieces // pair)
    def _(j):
        for c in (pair * j, pair * j + 1):
            first_relay(x_side, c)
        up_more(*[(t, pair * j + g) for t in (partner, shard(1, False)) for g in range(pair)])

    @pl.when(stage > 0)
    def _():
        send_part()

    @pl.when(stage == 0)
    def _():
        start_each(up_copy, visits[5:6] + visits[7:])
        for n in range(3):
            expand_panel(n)
        for t in visits[3:5]:
            up_copy(t).wait()

        @pl.when(inner)
        def _():
            up_copy(shard(3, False)).wait()

    @pl.loop(0, x_pieces // pair)
    def _(j):
        for c in (pair * j, pair * j + 1):
            second_relay(x_side, c)
        up_more(*[(t, pair * j + g) for t in (second_turn, shard(2, False)) for g in range(pair)])

    @pl.when(stage == 0)
    def _():
        start_each(down_copy, down_early)
        for n in range(3, a_pieces - 2):
            expand_panel(n)
        up_copy(second_other).wait()

        @pl.when(jnp.logical_not(inner))
        def _():
            up_copy(shard(3, False)).wait()

    for c in range(0, x_pieces - pair, pair):
        for g in range(pair):
            third_relay(x_side, c + g, True)
        up_more(*[(t, c + g) for t in (third_turn, second_other) for g in range(pair)])
    third_relay(x_side, end - 1, True)
    third_relay(x_side, end, False)

    @pl.when(stage == 0)
    def _():
        up_copy(last).wait()

    for c in range(end - 2):
        x_side.arrive(last, c)
    up_more((third_turn, end - 1), (third_turn, end), (second_other, end - 1), *[(last, c) for c in range(end - 2)])

    x_side.arrive(last, end - 2)
    end_extras(x_side)
    up_more((last, end - 2), (second_other, end), (last, end))

    others = partial.at[0:shards - 1]
    all_parts = pltpu.make_async_remote_copy(
        src_ref=others, dst_ref=others, send_sem=part_send.at[0], recv_sem=part_recv.at[0],
        device_id={"tp": me}, device_id_type=MESH)
    all_parts.wait_recv()

    summed = partial[0]
    for t in range(1, shards):
        summed = summed + partial[t]
    stacked = jnp.concatenate([summed] * segments + [jnp.zeros((LANES - segments * rank, LANES), f32)], axis=0)
    low = jnp.where(in_segment, jnp.transpose(stacked)[:rows], 0.0)

    x_side.arrive(last, end - 1)
    finals = [(last, end - 1)]
    square = sq[...]
    lefts = []
    for t, c in finals:
        wide = raw(t, c)
        square += squares(wide)
        lefts.append(scaled(t, c, wide))
    inverse = lax.rsqrt(jnp.sum(square, axis=1, keepdims=True) / width + EPSILON)
    low_rank = (low * inverse).astype(bf16)

    def up_finish(flipped):
        for n in range(a_pieces):
            block = slice(n * PIECE, (n + 1) * PIECE)
            base = jnp.zeros((rows, PIECE), f32)
            for (t, c), left in zip(finals, lefts):
                base += up_dot(left, n, t, c, flipped)
            adapted = lax.dot_general(low_rank, expand[block, :], NT, preferred_element_type=f32)
            value = inverse * (acc[:, block] + base) + adapted
            act[me, n] = (value / (1.0 + jnp.exp(-value))).astype(bf16)
            a_side.start_own(n)
            ready = a_pieces - 4 + n
            if n > 1 and a_pieces - 2 <= ready < a_pieces and not flipped:
                expand_panel(ready)

    per_stage(up_finish)

    def down_tile(n, t, c):
        at = pl.multiple_of(t * hidden + c * PIECE, LANES)
        return down_v[n * PIECE:(n + 1) * PIECE, pl.ds(at, PIECE)]

    def down_add(items):
        for n in range(x_pieces):
            block = slice(n * PIECE, (n + 1) * PIECE)
            part = jnp.zeros((rows, PIECE), f32)
            for t, c in items:
                part += lax.dot_general(act[t, c], down_tile(n, t, c), NT, preferred_element_type=f32)
            acc[:, block] = acc[:, block] + part

    @pl.when(stage == 0)
    def _():
        start_each(down_copy, down_late)

    for n in range(x_pieces):
        acc[:, n * PIECE:(n + 1) * PIECE] = xs[me, n].astype(f32)

    for t in down_early[:3]:
        down_copy(t).wait()
    end = a_pieces - 1

    @pl.loop(0, a_pieces)
    def _(c):
        first_relay(a_side, c)
        down_add([(me, c), (partner, c), (shard(1, False), c)])

    for t in down_early[3:]:
        down_copy(t).wait()

    @pl.loop(0, a_pieces)
    def _(c):
        second_relay(a_side, c)
        down_add([(second_turn, c), (shard(2, False), c)])

    for t in down_late:
        down_copy(t).wait()

    late = max(end - 2, 0)

    @pl.loop(0, late)
    def _(c):
        third_relay(a_side, c, True)
        down_add([(third_turn, c), (second_other, c)])

    @pl.loop(late, end)
    def _(c):
        third_relay(a_side, c, True)
        a_side.arrive(last, c - late)
        down_add([(third_turn, c), (second_other, c), (last, c - late)])

    third_relay(a_side, end, False)
    a_side.arrive(last, end - late)
    down_add([(third_turn, end), (last, end - late)])
    rest = list(range(end - late + 1, end - 1))
    for c in rest:
        a_side.arrive(last, c)
    down_add([(last, c) for c in rest])
    end_extras(a_side)
    down_add([(second_other, end), (last, end)])

    row = lax.broadcasted_iota(jnp.int32, (rows, 1), 0)
    kept = row < 0
    for s in range(segments):
        start = s * seg_rows
        kept = jnp.logical_or(kept, jnp.logical_and(row >= start, row < start + jnp.minimum(live_ref[s], seg_rows)))

    a_side.arrive(last, end - 1)
    for n in range(x_pieces):
        block = slice(n * PIECE, (n + 1) * PIECE)
        part = jnp.zeros((rows, PIECE), f32)
        part += lax.dot_general(act[last, end - 1], down_tile(n, last, end - 1), NT, preferred_element_type=f32)
        out_v[n] = jnp.where(kept, acc[:, block] + part, 0.0).astype(bf16)
        hand_each(n)
        out_copy(n).start()

    all_parts.wait_send()
    x_side.drain(act)
    a_side.drain(act)
    hand_drain()
    pltpu.make_async_copy(out_v, out_v, out_sem.at[0]).wait()


def fused_sections(current, ids, live, gain, up_weight, down_weight, shrink_weight, expand_weight):
    rows, cols = current.shape
    hidden = up_weight.shape[0]
    shards = lax.axis_size("tp")
    rank = shrink_weight.shape[1] // cols
    x_pieces, a_pieces = cols // PIECE, hidden // PIECE
    vmem = pl.BlockSpec(memory_space=pltpu.VMEM)
    smem = pl.BlockSpec(memory_space=pltpu.SMEM)
    hbm = pl.BlockSpec(memory_space=pl.ANY)
    dma = pltpu.SemaphoreType.DMA
    flat = PIECE * rank
    blocks = table_blocks(shards * hidden // flat * flat, shrink_weight) + a_pieces
    return pl.pallas_call(
        section_kernel,
        out_shape=jax.ShapeDtypeStruct((rows, cols), jnp.bfloat16),
        in_specs=[smem, smem, vmem] + [hbm] * 5,
        out_specs=hbm,
        scratch_shapes=[
            pltpu.VMEM(up_weight.shape, jnp.bfloat16),
            pltpu.VMEM(down_weight.shape, jnp.bfloat16),
            pltpu.VMEM((shards, x_pieces, rows, PIECE), jnp.bfloat16),
            pltpu.VMEM((shards, a_pieces, rows, PIECE), jnp.bfloat16),
            pltpu.VMEM((rows, hidden), jnp.float32),
            pltpu.VMEM((rows, LANES), jnp.float32),
            pltpu.VMEM((cols, LANES), jnp.bfloat16),
            pltpu.VMEM((hidden, LANES), jnp.bfloat16),
            pltpu.VMEM((shards, rank, LANES), jnp.float32),
            pltpu.VMEM((x_pieces, rows, PIECE), jnp.bfloat16),
            dma((shards,)), dma((shards,)), dma((blocks,)), dma((1,)),
            dma((1,)), dma((1,)),
            dma((4,)), dma((shards, x_pieces)),
            dma((4,)), dma((shards, a_pieces)),
            dma((1,)), dma((1,)),
        ],
        compiler_params=pltpu.CompilerParams(
            collective_id=0, has_side_effects=True, vmem_limit_bytes=VMEM_BYTES
        ),
    )(ids, live, gain[None, :], current, shrink_weight, expand_weight, up_weight, down_weight)


def table_blocks(width, *tables):
    return sum(-(-table.shape[1] // width) for table in tables)


def kernel_fits(row_count, col_count, hidden, segments, shrink_weight, expand_weight):
    shards = lax.axis_size("tp")
    adapters, flat_cols = shrink_weight.shape
    rank = flat_cols // col_count
    flat = PIECE * rank
    width = shards * hidden // flat * flat
    if col_count % PIECE or hidden % PIECE or hidden < 7 * PIECE or col_count // PIECE != 4:
        return False
    if row_count > LANES or rank * 8 != LANES or segments * rank > LANES or adapters % LANES:
        return False
    if shards != 4 * COLUMNS or col_count > hidden:
        return False
    if not width or hidden % LANES:
        return False
    whole, rest = flat // hidden, flat % hidden
    spots = 3 * (col_count // adapters - table_blocks(width, shrink_weight))
    pieces = hidden // PIECE
    if pieces * whole + (-(-pieces // (hidden // rest)) if rest else 0) > spots:
        return False
    return 2 * hidden * col_count * 2 * shards < VMEM_BYTES - 7 * 2**20


def run_window(
    units, unit_ids, unit_live, gain_full, up_weight, down_weight, shrink_weight, expand_weight
):
    section_index = lax.axis_index("pipe")
    sections = lax.axis_size("pipe")
    unit_count = units.shape[0]
    tick_total = unit_count + sections - 1

    def process(tick_index, received, collected):
        position = jnp.clip(tick_index - section_index, 0, unit_count - 1)
        arriving = lax.dynamic_index_in_dim(
            units, jnp.minimum(tick_index, unit_count - 1), 0, keepdims=False
        )
        current = jnp.where(section_index == 0, arriving, received)
        ids_here = lax.dynamic_index_in_dim(unit_ids, position, 0, keepdims=False)
        live_here = lax.dynamic_index_in_dim(unit_live, position, 0, keepdims=False)
        produced = block_step(
            current,
            ids_here,
            live_here,
            gain_full,
            up_weight,
            down_weight,
            shrink_weight,
            expand_weight,
        )
        lag = tick_index - section_index
        in_window = jnp.logical_and(lag >= 0, lag < unit_count)
        placed = lax.dynamic_update_index_in_dim(collected, produced, position, 0)
        return (produced, jnp.where(in_window, placed, collected))

    def one_tick(tick_index, state):
        produced, collected = process(tick_index, state[0], state[1])
        return (shifted(produced, "pipe", 1), collected)

    start_state = (jnp.zeros_like(units[0]), jnp.zeros_like(units))
    received, collected = lax.fori_loop(0, tick_total - 1, one_tick, start_state)
    produced, collected = process(tick_total - 1, received, collected)
    return collected


def per_device(
    hidden_entering,
    segment_adapter,
    segment_requests,
    section_norm_gain,
    up_matrix,
    down_matrix,
    adapter_reduce,
    adapter_expand,
):
    batch_list = hidden_entering.shape[0]
    row_count = hidden_entering.shape[1]
    col_count = hidden_entering.shape[2]
    hidden = up_matrix.shape[1]
    segments = segment_adapter.shape[1]
    if batch_list == 1 and kernel_fits(
        row_count, col_count, hidden, segments, adapter_reduce[0], adapter_expand[0]
    ):
        produced = fused_sections(
            hidden_entering[0],
            segment_adapter[0],
            segment_requests[0],
            section_norm_gain[0],
            up_matrix[0],
            down_matrix[0],
            adapter_reduce[0],
            adapter_expand[0],
        )
        return produced.reshape(1, batch_list, row_count, col_count)
    collected = run_window(
        hidden_entering,
        segment_adapter,
        segment_requests,
        section_norm_gain[0],
        up_matrix[0],
        down_matrix[0],
        adapter_reduce[0],
        adapter_expand[0],
    )
    return collected.reshape(1, batch_list, row_count, col_count)


def solution(mesh):
    return jax.shard_map(
        per_device,
        mesh=mesh,
        in_specs=(
            P("rep", None, "tp"),
            P("rep", None),
            P("rep", None),
            P("pipe", None),
            P("pipe", "tp", None),
            P("pipe", "tp", None),
            P("pipe", None, "tp"),
            P("pipe", None, "tp"),
        ),
        out_specs=P("pipe", "rep", None, "tp"),
        check_vma=False,
    )
```
